256 devices in a mesh: blk: 32 (over x, z), help: 8 (over y, core).
Axes of the slice: x: 4, y: 4, z: 8, core: 2. Of those that a mesh axis runs over, the one named last changes fastest.
Arguments:
- source_points: float32 [32, 1024, 128], P('blk'), may hold values from -4.5 to 4.5
- source_potential: float32 [32, 1024], P('blk'), may hold values from -3 to 3
- target_points: float32 [32, 1024, 128], P('blk', 'help'), may hold values from -4.5 to 4.5
- target_potential: float32 [32, 1024], P('blk', 'help'), may hold values from -3 to 3
- pairs: int32 [32, 16], P('blk'), may hold values from 0 to 31, as said below
- counts: int32 [32], P('blk'), may hold values from 1 to 16, as said below
- owner: int32 [32], replicated, may hold values from 0 to 31, each once
Outputs:
- new_source_points: float32 [32, 1024, 128], P('blk')
- new_source_potential: float32 [32, 1024], P('blk')
- new_target_points: float32 [32, 1024, 128], P('blk', 'help')
- new_target_potential: float32 [32, 1024], P('blk', 'help')
The draws below stay inside these ranges and needn't reach their ends.
Inputs may be any that keep to these rules, and one draw needn't show every extreme that they name: `pairs`: each row names 16 different clusters; every cluster is named in a live slot of some row. `counts`: every draw has a block with all 16 slots live.
All inputs are finite; a program needn't handle non-finite values.
Results may differ from the reference program's by a relative error of at most 0.019.
Values may be sent and summed in bfloat16 or wider, within the bound.
No kernel may reach another device: no remote copies, remote signals or barrier semaphores. Data moves between devices by JAX's collectives and lax.ppermute only.
A program may use at most 64 MiB of HBM per device.

```python
import jax
import jax.numpy as jnp
from jax import lax

E = 128
P_SIZE = 1024
Q = 512
ITERS = 2
NB = 32
PAIRS = 16


def draw_pairs(key, part):
    first_key, second_key = jax.random.split(jax.random.fold_in(key, 11))
    leader = jax.random.permutation(first_key, NB).astype(jnp.int32)
    scores = jax.random.randint(second_key, (NB, NB - 1), 0, 1 << 18) * NB + jnp.arange(NB - 1, dtype=jnp.int32)[None, :]
    order = jnp.argsort(scores, axis=1).astype(jnp.int32)
    offsets = jnp.concatenate([jnp.zeros((NB, 1), jnp.int32), order[:, :PAIRS - 1] + 1], axis=1)
    return ((leader[:, None] + offsets) % NB).astype(jnp.int32)


def draw_counts(key, part):
    first_key, second_key, third_key = jax.random.split(jax.random.fold_in(key, 23), 3)
    first = jax.random.randint(first_key, (NB,), 0, PAIRS)
    second = jax.random.randint(second_key, (NB,), 0, PAIRS)
    base = 1 + first * second // PAIRS
    chosen = jax.random.randint(third_key, (), 0, NB)
    return jnp.where(jnp.arange(NB) == chosen, PAIRS, base).astype(jnp.int32)


def level_of(own_key, shape, pieces, smallest, top_value):
    factor_of = 1.0
    for axis_at, blocks in pieces:
        draws = jax.random.uniform(jax.random.fold_in(jax.random.fold_in(own_key, 6), axis_at), (blocks,), jnp.float32, smallest / len(pieces), top_value / len(pieces))
        factor_of = factor_of * jnp.repeat(jnp.exp(draws), shape[axis_at] // blocks).reshape((-1,) + (1,) * (len(shape) - 1 - axis_at))
    return factor_of


def noise(rng, dims, spread, most, cuts=(), kind=jnp.bfloat16):
    level = level_of(rng, dims, cuts, -0.22, 0.18) if cuts else 1.0
    array = jax.random.normal(rng, dims, jnp.float32) * spread * level
    return jnp.minimum(jnp.maximum(array, -most), most).astype(kind)


def setup_inputs(seed: int = 0) -> dict:
    key_of = jax.random.split(jax.random.key(seed), 8)
    return {
        "source_points": noise(key_of[0], (NB, P_SIZE, E), 1.0, 4.5, ((0, 32),), jnp.float32),
        "source_potential": noise(key_of[1], (NB, P_SIZE), 0.5, 3.0, ((0, 32),), jnp.float32),
        "target_points": noise(key_of[2], (NB, P_SIZE, E), 1.0, 4.5, ((0, 32), (1, 8)), jnp.float32),
        "target_potential": noise(key_of[3], (NB, P_SIZE), 0.5, 3.0, ((0, 32), (1, 8)), jnp.float32),
        "pairs": draw_pairs(jax.random.fold_in(key_of[7], 71), 0),
        "counts": draw_counts(jax.random.fold_in(key_of[7], 71), 0),
        "owner": jax.random.permutation(key_of[6], NB).astype(jnp.int32),
    }


temper = 0.25
stride = 0.5
floor_value = -1e30


def combine(first, second):
    peak = jnp.maximum(first[0], second[0])
    left = jnp.exp(first[0] - peak)
    right = jnp.exp(second[0] - peak)
    return (peak, first[1] * left + second[1] * right, first[2] * left[..., None] + second[2] * right[..., None])


def tile_terms(src_block, src_square, src_level, tgt_block, tgt_square, tgt_level):
    width = src_block.shape[1]
    points = src_block.shape[0]
    row_peaks, row_sums, row_coords = [], [], []
    col_acc = None
    for start in range(0, points, Q):
        part_block = src_block[start:start + Q]
        part_square = src_square[start:start + Q]
        part_level = src_level[start:start + Q]
        cross = lax.dot_general(part_block, tgt_block, (((1,), (1,)), ((), ())), preferred_element_type=jnp.float32)
        cost = (part_square[:, None] + tgt_square[None, :] - 2.0 * cross) / width
        row_score = (tgt_level[None, :] - cost) / temper
        row_peak = jnp.max(row_score, axis=1)
        row_exp = jnp.exp(row_score - row_peak[:, None])
        row_peaks.append(row_peak)
        row_sums.append(jnp.sum(row_exp, axis=1))
        row_coords.append(jnp.dot(row_exp.astype(jnp.bfloat16), tgt_block, preferred_element_type=jnp.float32))
        col_score = (part_level[:, None] - cost) / temper
        col_peak = jnp.max(col_score, axis=0)
        col_exp = jnp.exp(col_score - col_peak[None, :])
        col_sum = jnp.sum(col_exp, axis=0)
        col_coord = lax.dot_general(col_exp.astype(jnp.bfloat16), part_block, (((0,), (0,)), ((), ())), preferred_element_type=jnp.float32)
        cols = (col_peak, col_sum, col_coord)
        col_acc = cols if col_acc is None else combine(col_acc, cols)
    rows = (jnp.concatenate(row_peaks), jnp.concatenate(row_sums), jnp.concatenate(row_coords, axis=0))
    return rows, col_acc


def blank_terms(count, width):
    return (jnp.full((count,), floor_value, jnp.float32), jnp.zeros((count,), jnp.float32), jnp.zeros((count, width), jnp.float32))


def sweep(source_points, source_potential, target_points, target_potential, partner, counts):
    blocks, points, width = source_points.shape
    src_round = source_points.astype(jnp.bfloat16)
    src_square = jnp.sum(jnp.square(src_round.astype(jnp.float32)), -1)
    tgt_round = target_points.astype(jnp.bfloat16)
    tgt_square = jnp.sum(jnp.square(tgt_round.astype(jnp.float32)), -1)
    col_init = (jnp.full((blocks, points), floor_value, jnp.float32), jnp.zeros((blocks, points), jnp.float32), jnp.zeros((blocks, points, width), jnp.float32))

    def per_block(col_acc, inputs):
        src_block, sq_block, level_block, partner_row, live_count = inputs

        def per_slot(carry, slot):
            row_acc, col_state = carry
            target_block = partner_row[slot].astype(jnp.int32)
            tgt_block = lax.dynamic_index_in_dim(tgt_round, target_block, 0, keepdims=False)
            tgt_sq = lax.dynamic_index_in_dim(tgt_square, target_block, 0, keepdims=False)
            tgt_lv = lax.dynamic_index_in_dim(target_potential, target_block, 0, keepdims=False)
            rows, cols = tile_terms(src_block, sq_block, level_block, tgt_block, tgt_sq, tgt_lv)
            live = slot < live_count
            blank = blank_terms(points, width)
            rows = tuple(jnp.where(live, value, empty) for value, empty in zip(rows, blank))
            cols = tuple(jnp.where(live, value, empty) for value, empty in zip(cols, blank))
            row_acc = combine(row_acc, rows)
            before = tuple(lax.dynamic_index_in_dim(value, target_block, 0, keepdims=False) for value in col_state)
            after = combine(before, cols)
            col_state = tuple(lax.dynamic_update_index_in_dim(value, fresh, target_block, 0) for value, fresh in zip(col_state, after))
            return (row_acc, col_state), None

        slots = jnp.arange(partner_row.shape[0], dtype=jnp.int32)
        (row_acc, col_acc), _ = lax.scan(per_slot, (blank_terms(points, width), col_acc), slots)
        return col_acc, row_acc

    col_acc, row_acc = lax.scan(per_block, col_init, (src_round, src_square, source_potential, partner, counts))
    row_peak, row_sum, row_coord = row_acc
    col_peak, col_sum, col_coord = col_acc
    new_source_potential = -temper * (row_peak + jnp.log(row_sum))
    new_source_points = source_points + stride * (row_coord / row_sum[..., None] - source_points)
    new_target_potential = -temper * (col_peak + jnp.log(col_sum))
    new_target_points = target_points + stride * (col_coord / col_sum[..., None] - target_points)
    return new_source_points, new_source_potential, new_target_points, new_target_potential


def reference(source_points, source_potential, target_points, target_potential, pairs, counts, owner):
    partner = jnp.take(owner, pairs, axis=0).astype(jnp.int32)
    state = (source_points, source_potential, target_points, target_potential)
    for step in range(ITERS):
        state = sweep(state[0], state[1], state[2], state[3], partner, counts)
    return (state[0], state[1], state[2], state[3])
```

```python
import jax
import jax.numpy as jnp
from jax import lax
from jax.experimental import pallas as pl
from jax.experimental.pallas import tpu as pltpu
from jax.sharding import Mesh
from jax.sharding import PartitionSpec as P

ITERS = 2
HELP = ("y", "c")
SHARD = 128
WIDTH = 128
SIDE = SHARD + 16
MSG = 2 * SIDE
META = 8
TEMPER = 0.25
STRIDE = 0.5
LOW = -1e30

F32 = jnp.float32
BF16 = jnp.bfloat16


def as_row(column):
    return jnp.broadcast_to(column, (SHARD, WIDTH)).T[:16]


def in_three(rows):
    hi = rows.astype(BF16)
    rest = rows - hi.astype(F32)
    mid = rest.astype(BF16)
    lo = (rest - mid.astype(F32)).astype(BF16)
    at = lax.broadcasted_iota(jnp.int32, rows.shape, 0)
    out = jnp.where(at == 0, hi.astype(F32), jnp.where(at == 1, mid.astype(F32), lo.astype(F32)))
    return jnp.where(at < 3, out, 0.0)


def of_three(rows):
    rows = rows.astype(F32)
    return rows[0:1] + rows[1:2] + rows[2:3]


def square_row(rounded):
    wide = rounded.astype(F32)
    return as_row(jnp.sum(wide * wide, axis=1, keepdims=True))


def write_side(msg_ref, side, points, level_row, meta=None):
    rounded = points.astype(BF16)
    bias = level_row * (1.0 / TEMPER) - square_row(rounded) * (1.0 / (WIDTH * TEMPER))
    extras = in_three(bias)
    if meta is not None:
        at = lax.broadcasted_iota(jnp.int32, extras.shape, 0)
        extras = jnp.where(at == META, meta, extras)
    msg_ref[pl.ds(side * SIDE, SHARD), :] = rounded
    msg_ref[pl.ds(side * SIDE + SHARD, 16), :] = extras.astype(BF16)


def prepare_kernel(pairs_ref, counts_ref, owner_ref, tp_ref, tl_ref, sp_ref, sl_ref, msg_ref):
    lane = lax.broadcasted_iota(jnp.int32, (1, WIDTH), 1)
    meta = jnp.zeros((1, WIDTH), F32)
    count = counts_ref[0]
    for slot in range(pairs_ref.shape[1]):
        partner = jnp.where(slot < count, owner_ref[pairs_ref[0, slot]], -1)
        meta = jnp.where(lane == partner, 1.0, meta)
    write_side(msg_ref, 0, tp_ref[...], tl_ref[...], meta)
    write_side(msg_ref, 1, sp_ref[...], sl_ref[...])


def attend_kernel(mask_ref, keys_ref, query_ref, out_ref, scaled_ref, peak_ref, sum_ref, acc_ref):
    blocks = keys_ref.shape[0]
    helpers = query_ref.shape[0]
    for side in range(2):
        q_at = side * SIDE
        k_at = (1 - side) * SIDE
        for c in range(helpers):
            rows = pl.ds(c * SHARD, SHARD)
            scaled_ref[rows, :] = query_ref[c, pl.ds(q_at, SHARD), :] * jnp.asarray(
                2.0 / (WIDTH * TEMPER), BF16
            )
        peak_ref[...] = jnp.full(peak_ref.shape, LOW, F32)
        sum_ref[...] = jnp.zeros(sum_ref.shape, F32)
        acc_ref[...] = jnp.zeros(acc_ref.shape, F32)

        def scores(j, c):
            key = keys_ref[j, pl.ds(k_at, SHARD), :]
            bias = of_three(keys_ref[j, pl.ds(k_at + SHARD, 16), :])
            cross = lax.dot_general(
                scaled_ref[pl.ds(c * SHARD, SHARD), :],
                key,
                (((1,), (1,)), ((), ())),
                preferred_element_type=F32,
            )
            return cross + bias, key

        def find_peak(j, carry):
            @pl.when(mask_ref[side, j] > 0)
            def _():
                for c in range(helpers):
                    rows = pl.ds(c * SHARD, SHARD)
                    peak_ref[rows, :] = jnp.maximum(peak_ref[rows, :], scores(j, c)[0])

            return carry

        lax.fori_loop(0, blocks, find_peak, 0)
        for c in range(helpers):
            rows = pl.ds(c * SHARD, SHARD)
            top = jnp.max(peak_ref[rows, :], axis=1, keepdims=True)
            peak_ref[rows, :] = jnp.broadcast_to(top, (SHARD, WIDTH))

        def add_up(j, carry):
            @pl.when(mask_ref[side, j] > 0)
            def _():
                for c in range(helpers):
                    rows = pl.ds(c * SHARD, SHARD)
                    score, key = scores(j, c)
                    weight = jnp.exp(score - peak_ref[rows, :])
                    sum_ref[rows, :] += weight
                    acc_ref[rows, :] += jnp.dot(
                        weight.astype(BF16), key, preferred_element_type=F32
                    )

            return carry

        lax.fori_loop(0, blocks, add_up, 0)
        for c in range(helpers):
            rows = pl.ds(c * SHARD, SHARD)
            total = jnp.sum(sum_ref[rows, :], axis=1, keepdims=True)
            lse = peak_ref[rows, :][:, 0:1] + jnp.log(total)
            out_ref[c, pl.ds(q_at, SHARD), :] = (acc_ref[rows, :] / total).astype(BF16)
            out_ref[c, pl.ds(q_at + SHARD, 16), :] = in_three(as_row(lse)).astype(BF16)


def settle_kernel(got_ref, tp_ref, sp_ref, ntp_ref, ntl_ref, nsp_ref, nsl_ref, msg_ref, scr_ref):
    helpers = got_ref.shape[0]
    sides = ((0, tp_ref, ntp_ref, ntl_ref), (1, sp_ref, nsp_ref, nsl_ref))
    for side, old_ref, new_ref, level_ref in sides:
        at = side * SIDE
        parts = [of_three(got_ref[h, pl.ds(at + SHARD, 16), :]) for h in range(helpers)]
        top = parts[0]
        for part in parts[1:]:
            top = jnp.maximum(top, part)
        shares = [jnp.exp(part - top) for part in parts]
        total = shares[0]
        for share in shares[1:]:
            total = total + share
        scr_ref[...] = jnp.zeros(scr_ref.shape, F32)
        for h in range(helpers):
            scr_ref[pl.ds(h, 1), :] = shares[h] / total
        columns = scr_ref[...].T
        mean = jnp.zeros((SHARD, WIDTH), F32)
        for h in range(helpers):
            mean = mean + columns[:, h : h + 1] * got_ref[h, pl.ds(at, SHARD), :].astype(F32)
        old = old_ref[...]
        square = square_row(old.astype(BF16))
        level = -TEMPER * (top + jnp.log(total) - square * (1.0 / (WIDTH * TEMPER)))
        new = old + STRIDE * (mean - old)
        new_ref[...] = new
        level_ref[...] = level[:8]
        write_side(msg_ref, side, new, level)


def gathered(x, axes):
    copies = jnp.broadcast_to(x, (lax.axis_size(axes), *x.shape))
    return lax.all_to_all(copies, axes, split_axis=0, concat_axis=0, tiled=True)


def on_device(
    source_points, source_potential, target_points, target_potential, pairs, counts, owner
):
    helper = lax.axis_index(HELP)
    block = lax.axis_index(("x", "z"))
    blocks = lax.axis_size(("x", "z"))
    helpers = lax.axis_size(HELP)
    tp = target_points[0]
    sp = lax.dynamic_slice_in_dim(source_points[0], helper * SHARD, SHARD, 0)
    sl = lax.dynamic_slice_in_dim(source_potential, helper * SHARD, SHARD, 1)
    smem = pl.BlockSpec(memory_space=pltpu.SMEM)
    vmem = pl.BlockSpec(memory_space=pltpu.VMEM)
    msg_shape = jax.ShapeDtypeStruct((MSG, WIDTH), BF16)
    msg = pl.pallas_call(
        prepare_kernel,
        out_shape=msg_shape,
        in_specs=[smem, smem, smem, vmem, vmem, vmem, vmem],
        out_specs=vmem,
        name="prepare",
    )(pairs, counts, owner, tp, target_potential, sp, sl)
    points_shape = jax.ShapeDtypeStruct((SHARD, WIDTH), F32)
    level_shape = jax.ShapeDtypeStruct((8, SHARD), F32)
    mask = None
    for step in range(ITERS):
        near = gathered(msg, "z")
        keys = gathered(near, "x").reshape(blocks, MSG, WIDTH)
        query = gathered(msg, HELP)
        if mask is None:
            named = keys[:, SHARD + META, :blocks]
            by_source = lax.dynamic_slice_in_dim(named, block, 1, 0)[0]
            by_target = lax.dynamic_slice_in_dim(named, block, 1, 1)[:, 0]
            mask = jnp.stack([by_target, by_source]).astype(jnp.int32)
        parts = pl.pallas_call(
            attend_kernel,
            out_shape=jax.ShapeDtypeStruct((helpers, MSG, WIDTH), BF16),
            in_specs=[smem, vmem, vmem],
            out_specs=vmem,
            scratch_shapes=[
                pltpu.VMEM((helpers * SHARD, WIDTH), BF16),
                pltpu.VMEM((helpers * SHARD, WIDTH), F32),
                pltpu.VMEM((helpers * SHARD, WIDTH), F32),
                pltpu.VMEM((helpers * SHARD, WIDTH), F32),
            ],
            name="attend",
        )(mask, keys, query)
        got = lax.all_to_all(parts, HELP, split_axis=0, concat_axis=0, tiled=True)
        tp, tl, sp, sl, msg = pl.pallas_call(
            settle_kernel,
            out_shape=(points_shape, level_shape, points_shape, level_shape, msg_shape),
            in_specs=[vmem, vmem, vmem],
            out_specs=(vmem, vmem, vmem, vmem, vmem),
            scratch_shapes=[pltpu.VMEM((WIDTH, SHARD), F32)],
            name="settle",
        )(got, tp, sp)
    done = gathered(jnp.concatenate([sp, sl], axis=0), HELP)
    new_source_points = done[:, :SHARD].reshape(1, helpers * SHARD, WIDTH)
    new_source_potential = done[:, SHARD].reshape(1, helpers * SHARD)
    return new_source_points, new_source_potential, tp[None], tl[:1]


def solution(mesh):
    torus = Mesh(mesh.devices.reshape(4, 8, 4, 2), ("x", "z", "y", "c"))
    blk = ("x", "z")
    in_specs = (
        P(blk, None, None),
        P(blk, None),
        P(blk, HELP, None),
        P(blk, HELP),
        P(blk, None),
        P(blk),
        P(),
    )
    out_specs = (P(blk, None, None), P(blk, None), P(blk, HELP, None), P(blk, HELP))
    return jax.shard_map(
        on_device, mesh=torus, in_specs=in_specs, out_specs=out_specs, check_vma=False
    )
```

```python
import jax
import jax.numpy as jnp
from jax import lax
from jax.experimental import pallas as pl
from jax.experimental.pallas import tpu as pltpu
from jax.sharding import Mesh
from jax.sharding import PartitionSpec as P

ITERS = 2
HELP = ("y", "c")
SHARD = 128
WIDTH = 128
SIDE = SHARD + 16
MSG = 2 * SIDE
META = 8
TEMPER = 0.25
STRIDE = 0.5
LOW = -1e30

F32 = jnp.float32
BF16 = jnp.bfloat16


def as_row(column):
    return jnp.broadcast_to(column, (SHARD, WIDTH)).T[:16]


def in_three(rows):
    hi = rows.astype(BF16)
    rest = rows - hi.astype(F32)
    mid = rest.astype(BF16)
    lo = (rest - mid.astype(F32)).astype(BF16)
    at = lax.broadcasted_iota(jnp.int32, rows.shape, 0)
    out = jnp.where(at == 0, hi.astype(F32), jnp.where(at == 1, mid.astype(F32), lo.astype(F32)))
    return jnp.where(at < 3, out, 0.0)


def of_three(rows):
    rows = rows.astype(F32)
    return rows[0:1] + rows[1:2] + rows[2:3]


def square_row(rounded):
    wide = rounded.astype(F32)
    return as_row(jnp.sum(wide * wide, axis=1, keepdims=True))


def write_side(msg_ref, copies_ref, side, points, level_row, meta=None):
    rounded = points.astype(BF16)
    bias = level_row * (1.0 / TEMPER) - square_row(rounded) * (1.0 / (WIDTH * TEMPER))
    extras = in_three(bias)
    if meta is not None:
        at = lax.broadcasted_iota(jnp.int32, extras.shape, 0)
        extras = jnp.where(at == META, meta, extras)
    extras = extras.astype(BF16)
    msg_ref[pl.ds(side * SIDE, SHARD), :] = rounded
    msg_ref[pl.ds(side * SIDE + SHARD, 16), :] = extras
    for k in range(copies_ref.shape[0]):
        copies_ref[k, pl.ds(side * SIDE, SHARD), :] = rounded
        copies_ref[k, pl.ds(side * SIDE + SHARD, 16), :] = extras


def prepare_kernel(
    at_ref, pairs_ref, counts_ref, owner_ref, tp_ref, tl_ref, sp_ref, sl_ref, msg_ref, copies_ref
):
    lane = lax.broadcasted_iota(jnp.int32, (1, WIDTH), 1)
    meta = jnp.zeros((1, WIDTH), F32)
    count = counts_ref[0]
    for slot in range(pairs_ref.shape[1]):
        partner = jnp.where(slot < count, owner_ref[pairs_ref[0, slot]], -1)
        meta = jnp.where(lane == partner, 1.0, meta)
    write_side(msg_ref, copies_ref, 0, tp_ref[0], tl_ref[...], meta)
    write_side(msg_ref, copies_ref, 1, sp_ref[0], sl_ref[...])


def attend_kernel(mask_ref, place_ref, keys_ref, *refs):
    helpers = place_ref.shape[0]
    query_refs, (out_ref, list_ref, scaled_ref, peak_ref, sum_ref, acc_ref) = refs[:helpers], refs[helpers:]
    blocks = keys_ref.shape[0]
    for side in range(2):
        q_at = side * SIDE
        k_at = (1 - side) * SIDE

        def enlist(j, count):
            list_ref[count] = j
            return count + jnp.where(mask_ref[side, j] > 0, 1, 0)

        live = lax.fori_loop(0, blocks, enlist, 0)
        list_ref[live] = list_ref[0]
        for c in range(helpers):
            scaled_ref[pl.ds(c * SHARD, SHARD), :] = query_refs[c][pl.ds(q_at, SHARD), :] * jnp.asarray(
                2.0 / (WIDTH * TEMPER), BF16
            )
        peak_ref[...] = jnp.full(peak_ref.shape, LOW, F32)
        sum_ref[...] = jnp.zeros(sum_ref.shape, F32)
        acc_ref[...] = jnp.zeros(acc_ref.shape, F32)

        def scores(t):
            first = list_ref[2 * t]
            second = list_ref[2 * t + 1]
            key = jnp.concatenate(
                [keys_ref[first, pl.ds(k_at, SHARD), :], keys_ref[second, pl.ds(k_at, SHARD), :]], axis=0
            )
            left = of_three(keys_ref[first, pl.ds(k_at + SHARD, 16), :])
            right = of_three(keys_ref[second, pl.ds(k_at + SHARD, 16), :])
            right = jnp.where(2 * t + 1 < live, right, LOW)
            cross = lax.dot_general(
                scaled_ref[...], key, (((1,), (1,)), ((), ())), preferred_element_type=F32
            )
            return cross[:, :SHARD] + left, cross[:, SHARD:] + right, key

        def find_peak(t, carry):
            left, right, _ = scores(t)
            peak_ref[...] = jnp.maximum(peak_ref[...], jnp.maximum(left, right))
            return carry

        def add_up(t, carry):
            left, right, key = scores(t)
            peak = peak_ref[...]
            left = jnp.exp(left - peak)
            right = jnp.exp(right - peak)
            sum_ref[...] += left + right
            weight = jnp.concatenate([left.astype(BF16), right.astype(BF16)], axis=1)
            acc_ref[...] += jnp.dot(weight, key, preferred_element_type=F32)
            return carry

        turns = (live + 1) // 2
        lax.fori_loop(0, turns, find_peak, 0)
        for c in range(helpers):
            rows = pl.ds(c * SHARD, SHARD)
            top = jnp.max(peak_ref[rows, :], axis=1, keepdims=True)
            peak_ref[rows, :] = jnp.broadcast_to(top, (SHARD, WIDTH))
        lax.fori_loop(0, turns, add_up, 0)
        for c in range(helpers):
            rows = pl.ds(c * SHARD, SHARD)
            total = jnp.sum(sum_ref[rows, :], axis=1, keepdims=True)
            lse = peak_ref[rows, :][:, 0:1] + jnp.log(total)
            to = place_ref[c]
            out_ref[to, pl.ds(q_at, SHARD), :] = (acc_ref[rows, :] * (1.0 / total)).astype(BF16)
            out_ref[to, pl.ds(q_at + SHARD, 16), :] = in_three(as_row(lse)).astype(BF16)


def settle_kernel(got_ref, tp_ref, sp_ref, ntp_ref, ntl_ref, nsp_ref, nsl_ref, msg_ref, copies_ref, scr_ref):
    helpers = got_ref.shape[0]
    sides = ((0, tp_ref, ntp_ref, ntl_ref), (1, sp_ref, nsp_ref, nsl_ref))
    for side, old_ref, new_ref, level_ref in sides:
        at = side * SIDE
        parts = [of_three(got_ref[h, pl.ds(at + SHARD, 16), :]) for h in range(helpers)]
        top = parts[0]
        for part in parts[1:]:
            top = jnp.maximum(top, part)
        shares = [jnp.exp(part - top) for part in parts]
        total = shares[0]
        for share in shares[1:]:
            total = total + share
        scr_ref[...] = jnp.zeros(scr_ref.shape, F32)
        for h in range(helpers):
            scr_ref[pl.ds(h, 1), :] = shares[h] / total
        columns = scr_ref[...].T
        mean = jnp.zeros((SHARD, WIDTH), F32)
        for h in range(helpers):
            mean = mean + columns[:, h : h + 1] * got_ref[h, pl.ds(at, SHARD), :].astype(F32)
        old = old_ref[...]
        square = square_row(old.astype(BF16))
        level = -TEMPER * (top + jnp.log(total) - square * (1.0 / (WIDTH * TEMPER)))
        new = old + STRIDE * (mean - old)
        new_ref[...] = new
        level_ref[...] = level[:8]
        write_side(msg_ref, copies_ref, side, new, level)


def gathered(x, axes):
    copies = jnp.broadcast_to(x, (lax.axis_size(axes), *x.shape))
    return lax.all_to_all(copies, axes, split_axis=0, concat_axis=0, tiled=True)


def exchanged(copies, axes):
    return lax.all_to_all(copies, axes, split_axis=0, concat_axis=0, tiled=True)


def from_helpers(msg):
    ring = lax.axis_size("y")
    swap = [(0, 1), (1, 0)]
    pieces = []
    for k in range(ring):
        piece = msg if k == 0 else lax.ppermute(msg, "y", [(i, (i + k) % ring) for i in range(ring)])
        pieces += [piece, lax.ppermute(piece, "c", swap)]
    return pieces


def on_device(
    source_points, source_potential, target_points, target_potential, pairs, counts, owner
):
    helper = lax.axis_index(HELP)
    block = lax.axis_index(("x", "z"))
    blocks = lax.axis_size(("x", "z"))
    helpers = lax.axis_size(HELP)
    ring = lax.axis_size("y")
    row, core = lax.axis_index("y"), lax.axis_index("c")
    place = jnp.stack([(row - k) % ring * 2 + (core + n) % 2 for k in range(ring) for n in range(2)])
    smem = pl.BlockSpec(memory_space=pltpu.SMEM)
    vmem = pl.BlockSpec(memory_space=pltpu.VMEM)
    msg_shape = jax.ShapeDtypeStruct((MSG, WIDTH), BF16)
    copies_shape = jax.ShapeDtypeStruct((lax.axis_size("z"), MSG, WIDTH), BF16)
    own_points = pl.BlockSpec((1, SHARD, WIDTH), lambda i, at: (0, at[0], 0))
    own_level = pl.BlockSpec((1, SHARD), lambda i, at: (0, at[0]))
    whole = lambda *shape: pl.BlockSpec(shape, lambda i, at: (0,) * len(shape))
    msg, copies = pl.pallas_call(
        prepare_kernel,
        out_shape=(msg_shape, copies_shape),
        grid_spec=pltpu.PrefetchScalarGridSpec(
            num_scalar_prefetch=1,
            grid=(1,),
            in_specs=[smem, smem, smem, whole(1, SHARD, WIDTH), whole(1, SHARD), own_points, own_level],
            out_specs=(whole(*msg_shape.shape), whole(*copies_shape.shape)),
        ),
        name="prepare",
    )(helper[None], pairs, counts, owner, target_points, target_potential, source_points, source_potential)
    tp = target_points[0]
    sp = lax.dynamic_slice_in_dim(source_points[0], helper * SHARD, SHARD, 0)
    points_shape = jax.ShapeDtypeStruct((SHARD, WIDTH), F32)
    level_shape = jax.ShapeDtypeStruct((8, SHARD), F32)
    mask = None
    for step in range(ITERS):
        near = exchanged(copies, "z")
        keys = gathered(near, "x").reshape(blocks, MSG, WIDTH)
        query = from_helpers(msg)
        if mask is None:
            named = keys[:, SHARD + META, :blocks]
            by_source = lax.dynamic_slice_in_dim(named, block, 1, 0)[0]
            by_target = lax.dynamic_slice_in_dim(named, block, 1, 1)[:, 0]
            mask = jnp.stack([by_target, by_source]).astype(jnp.int32)
        parts = pl.pallas_call(
            attend_kernel,
            out_shape=jax.ShapeDtypeStruct((helpers, MSG, WIDTH), BF16),
            in_specs=[smem, smem, vmem] + [vmem] * helpers,
            out_specs=vmem,
            scratch_shapes=[
                pltpu.SMEM((blocks + 1,), jnp.int32),
                pltpu.VMEM((helpers * SHARD, WIDTH), BF16),
                pltpu.VMEM((helpers * SHARD, WIDTH), F32),
                pltpu.VMEM((helpers * SHARD, WIDTH), F32),
                pltpu.VMEM((helpers * SHARD, WIDTH), F32),
            ],
            name="attend",
        )(mask, place, keys, *query)
        got = exchanged(parts, HELP)
        tp, tl, sp, sl, msg, copies = pl.pallas_call(
            settle_kernel,
            out_shape=(points_shape, level_shape, points_shape, level_shape, msg_shape, copies_shape),
            in_specs=[vmem, vmem, vmem],
            out_specs=(vmem,) * 6,
            scratch_shapes=[pltpu.VMEM((WIDTH, SHARD), F32)],
            name="settle",
        )(got, tp, sp)
    done = gathered(jnp.concatenate([sp, sl], axis=0), HELP)
    new_source_points = done[:, :SHARD].reshape(1, helpers * SHARD, WIDTH)
    new_source_potential = done[:, SHARD].reshape(1, helpers * SHARD)
    return new_source_points, new_source_potential, tp[None], tl[:1]


def solution(mesh):
    torus = Mesh(mesh.devices.reshape(4, 8, 4, 2), ("x", "z", "y", "c"))
    blk = ("x", "z")
    in_specs = (
        P(blk, None, None),
        P(blk, None),
        P(blk, HELP, None),
        P(blk, HELP),
        P(blk, None),
        P(blk),
        P(),
    )
    out_specs = (P(blk, None, None), P(blk, None), P(blk, HELP, None), P(blk, HELP))
    return jax.shard_map(
        on_device, mesh=torus, in_specs=in_specs, out_specs=out_specs, check_vma=False
    )
```

```python
import jax
import jax.numpy as jnp
from jax import lax
from jax.experimental import pallas as pl
from jax.experimental.pallas import tpu as pltpu
from jax.sharding import Mesh
from jax.sharding import PartitionSpec as P

ITERS = 2
HELP = ("y", "c")
SHARD = 128
WIDTH = 128
SIDE = SHARD + 16
MSG = 2 * SIDE
META = 8
XS, ZS, YS, CS = 4, 8, 4, 2
TEMPER = 0.25
STRIDE = 0.5
LOW = -1e30

F32 = jnp.float32
BF16 = jnp.bfloat16


def as_row(column):
    return jnp.broadcast_to(column, (SHARD, WIDTH)).T[:16]


def in_three(rows):
    hi = rows.astype(BF16)
    rest = rows - hi.astype(F32)
    mid = rest.astype(BF16)
    lo = (rest - mid.astype(F32)).astype(BF16)
    at = lax.broadcasted_iota(jnp.int32, rows.shape, 0)
    out = jnp.where(at == 0, hi.astype(F32), jnp.where(at == 1, mid.astype(F32), lo.astype(F32)))
    return jnp.where(at < 3, out, 0.0)


def of_three(rows):
    rows = rows.astype(F32)
    return rows[0:1] + rows[1:2] + rows[2:3]


def square_row(rounded):
    wide = rounded.astype(F32)
    return as_row(jnp.sum(wide * wide, axis=1, keepdims=True))


def write_side(msg_ref, copies_ref, source_ref, side, points, level_row, meta=None):
    rounded = points.astype(BF16)
    bias = level_row * (1.0 / TEMPER) - square_row(rounded) * (1.0 / (WIDTH * TEMPER))
    extras = in_three(bias)
    if meta is not None:
        at = lax.broadcasted_iota(jnp.int32, extras.shape, 0)
        extras = jnp.where(at == META, meta, extras)
    extras = extras.astype(BF16)
    msg_ref[pl.ds(side * SIDE, SHARD), :] = rounded
    msg_ref[pl.ds(side * SIDE + SHARD, 16), :] = extras
    if side == 0:
        for k in range(copies_ref.shape[0]):
            copies_ref[k, pl.ds(0, SHARD), :] = rounded
            copies_ref[k, pl.ds(SHARD, 16), :] = extras
    else:
        source_ref[pl.ds(0, SHARD), :] = rounded
        source_ref[pl.ds(SHARD, 16), :] = extras


def prepare_kernel(
    at_ref, pairs_ref, counts_ref, owner_ref, tp_ref, tl_ref, sp_ref, sl_ref, msg_ref, copies_ref, source_ref
):
    lane = lax.broadcasted_iota(jnp.int32, (1, WIDTH), 1)
    meta = jnp.zeros((1, WIDTH), F32)
    count = counts_ref[0]
    for slot in range(pairs_ref.shape[1]):
        partner = jnp.where(slot < count, owner_ref[pairs_ref[0, slot]], -1)
        meta = jnp.where(lane == partner, 1.0, meta)
    write_side(msg_ref, copies_ref, source_ref, 0, tp_ref[0], tl_ref[...], meta)
    write_side(msg_ref, copies_ref, source_ref, 1, sp_ref[0], sl_ref[...])


def attend_kernel(at_ref, pairs_ref, counts_ref, owner_ref, named_ref, *refs):
    far, ring, helpers = XS, ZS, YS * CS
    target_refs, refs = refs[:far], refs[far:]
    source_refs, refs = refs[:ring], refs[ring:]
    query_refs, refs = refs[:helpers], refs[helpers:]
    out_ref, list_ref, key_ref, scaled_ref, peak_ref, sum_ref, acc_ref = refs
    at_x, at_z, at_y, at_c = at_ref[0], at_ref[1], at_ref[2], at_ref[3]
    blocks = far * ring
    for k in range(ring):
        key_ref[pl.ds(k * far, far)] = source_refs[k][...]
    for k in range(far):
        key_ref[pl.ds(blocks + k * ring, ring)] = target_refs[k][...]

    def enlist_sources(j, count):
        list_ref[0, count] = ((at_z - j) & (ring - 1)) * far + j // ring
        return count + jnp.where(named_ref[j] > 0, 1, 0)

    def enlist_targets(s, carry):
        block = owner_ref[pairs_ref[0, s]]
        list_ref[1, s] = blocks + ((at_x - block // ring) & (far - 1)) * ring + (block & (ring - 1))
        return carry

    naming = lax.fori_loop(0, blocks, enlist_sources, 0)
    lax.fori_loop(0, pairs_ref.shape[1], enlist_targets, 0)

    def one_side(side, carry):
        q_at = pl.multiple_of(side * SIDE, 16)
        live = jnp.where(side == 0, naming, counts_ref[0])
        list_ref[side, live] = list_ref[side, 0]
        for c in range(helpers):
            scaled_ref[pl.ds(c * SHARD, SHARD), :] = query_refs[c][pl.ds(q_at, SHARD), :] * jnp.asarray(
                2.0 / (WIDTH * TEMPER), BF16
            )
        peak_ref[...] = jnp.full(peak_ref.shape, LOW, F32)
        sum_ref[...] = jnp.zeros(sum_ref.shape, F32)
        acc_ref[...] = jnp.zeros(acc_ref.shape, F32)

        def scores(t):
            first = list_ref[side, 2 * t]
            second = list_ref[side, 2 * t + 1]
            key = jnp.concatenate([key_ref[first, pl.ds(0, SHARD), :], key_ref[second, pl.ds(0, SHARD), :]], axis=0)
            left = of_three(key_ref[first, pl.ds(SHARD, 16), :])
            right = of_three(key_ref[second, pl.ds(SHARD, 16), :])
            right = jnp.where(2 * t + 1 < live, right, LOW)
            cross = lax.dot_general(
                scaled_ref[...], key, (((1,), (1,)), ((), ())), preferred_element_type=F32
            )
            return cross[:, :SHARD] + left, cross[:, SHARD:] + right, key

        def find_peak(t, carry):
            left, right, _ = scores(t)
            peak_ref[...] = jnp.maximum(peak_ref[...], jnp.maximum(left, right))
            return carry

        def add_up(t, carry):
            left, right, key = scores(t)
            peak = peak_ref[...]
            left = jnp.exp(left - peak)
            right = jnp.exp(right - peak)
            sum_ref[...] += left + right
            weight = jnp.concatenate([left.astype(BF16), right.astype(BF16)], axis=1)
            acc_ref[...] += jnp.dot(weight, key, preferred_element_type=F32)
            return carry

        turns = (live + 1) // 2
        lax.fori_loop(0, turns, find_peak, 0)
        for c in range(helpers):
            rows = pl.ds(c * SHARD, SHARD)
            top = jnp.max(peak_ref[rows, :], axis=1, keepdims=True)
            peak_ref[rows, :] = jnp.broadcast_to(top, (SHARD, WIDTH))
        lax.fori_loop(0, turns, add_up, 0)
        for c in range(helpers):
            rows = pl.ds(c * SHARD, SHARD)
            total = jnp.sum(sum_ref[rows, :], axis=1, keepdims=True)
            lse = peak_ref[rows, :][:, 0:1] + jnp.log(total)
            to = ((at_y - c // CS) & (YS - 1)) * CS + ((at_c + c) & (CS - 1))
            out_ref[to, pl.ds(q_at, SHARD), :] = (acc_ref[rows, :] * (1.0 / total)).astype(BF16)
            out_ref[to, pl.ds(pl.multiple_of(q_at + SHARD, 16), 16), :] = in_three(as_row(lse)).astype(BF16)
        return carry

    lax.fori_loop(0, 2, one_side, 0)


def settle_kernel(got_ref, tp_ref, sp_ref, ntp_ref, ntl_ref, nsp_ref, nsl_ref, msg_ref, copies_ref, source_ref, scr_ref):
    helpers = got_ref.shape[0]
    sides = ((0, tp_ref, ntp_ref, ntl_ref), (1, sp_ref, nsp_ref, nsl_ref))
    for side, old_ref, new_ref, level_ref in sides:
        at = side * SIDE
        parts = [of_three(got_ref[h, pl.ds(at + SHARD, 16), :]) for h in range(helpers)]
        top = parts[0]
        for part in parts[1:]:
            top = jnp.maximum(top, part)
        shares = [jnp.exp(part - top) for part in parts]
        total = shares[0]
        for share in shares[1:]:
            total = total + share
        scr_ref[...] = jnp.zeros(scr_ref.shape, F32)
        for h in range(helpers):
            scr_ref[pl.ds(h, 1), :] = shares[h] / total
        columns = scr_ref[...].T
        mean = jnp.zeros((SHARD, WIDTH), F32)
        for h in range(helpers):
            mean = mean + columns[:, h : h + 1] * got_ref[h, pl.ds(at, SHARD), :].astype(F32)
        old = old_ref[...]
        square = square_row(old.astype(BF16))
        level = -TEMPER * (top + jnp.log(total) - square * (1.0 / (WIDTH * TEMPER)))
        new = old + STRIDE * (mean - old)
        new_ref[...] = new
        level_ref[...] = level[:8]
        write_side(msg_ref, copies_ref, source_ref, side, new, level)


def gathered(x, axes):
    copies = jnp.broadcast_to(x, (lax.axis_size(axes), *x.shape))
    return lax.all_to_all(copies, axes, split_axis=0, concat_axis=0, tiled=True)


def exchanged(copies, axes):
    return lax.all_to_all(copies, axes, split_axis=0, concat_axis=0, tiled=True)


def shifted(x, axis, step):
    n = lax.axis_size(axis)
    return lax.ppermute(x, axis, [(i, (i + step) % n) for i in range(n)])


def from_helpers(msg):
    pieces = []
    for k in range(YS):
        piece = shifted(msg, "y", k) if k else msg
        pieces += [piece, shifted(piece, "c", 1)]
    return pieces


def from_blocks(copies, source):
    sides = [source] + [shifted(source, "x", k) for k in range(1, XS)]
    near = exchanged(copies, "z")
    ring = [None] * ZS
    ring[0] = ahead = back = jnp.stack(sides)
    targets = [near]
    for k in range(1, XS):
        targets.append(shifted(near, "x", k))
    for k in range(1, ZS // 2 + 1):
        ring[k] = ahead = shifted(ahead, "z", 1)
        if k < ZS // 2:
            ring[ZS - k] = back = shifted(back, "z", ZS - 1)
    return targets, ring


def on_device(
    source_points, source_potential, target_points, target_potential, pairs, counts, owner
):
    helper = lax.axis_index(HELP)
    block = lax.axis_index(("x", "z"))
    blocks = XS * ZS
    helpers = YS * CS
    at = jnp.stack([lax.axis_index(axis) for axis in ("x", "z", "y", "c")])
    smem = pl.BlockSpec(memory_space=pltpu.SMEM)
    vmem = pl.BlockSpec(memory_space=pltpu.VMEM)
    msg_shape = jax.ShapeDtypeStruct((MSG, WIDTH), BF16)
    copies_shape = jax.ShapeDtypeStruct((ZS, SIDE, WIDTH), BF16)
    source_shape = jax.ShapeDtypeStruct((SIDE, WIDTH), BF16)
    own_points = pl.BlockSpec((1, SHARD, WIDTH), lambda i, at: (0, at[2] * CS + at[3], 0))
    own_level = pl.BlockSpec((1, SHARD), lambda i, at: (0, at[2] * CS + at[3]))
    whole = lambda *shape: pl.BlockSpec(shape, lambda i, at: (0,) * len(shape))
    msg, copies, source = pl.pallas_call(
        prepare_kernel,
        out_shape=(msg_shape, copies_shape, source_shape),
        grid_spec=pltpu.PrefetchScalarGridSpec(
            num_scalar_prefetch=1,
            grid=(1,),
            in_specs=[smem, smem, smem, whole(1, SHARD, WIDTH), whole(1, SHARD), own_points, own_level],
            out_specs=(whole(*msg_shape.shape), whole(*copies_shape.shape), whole(*source_shape.shape)),
        ),
        name="prepare",
    )(at, pairs, counts, owner, target_points, target_potential, source_points, source_potential)
    tp = target_points[0]
    sp = lax.dynamic_slice_in_dim(source_points[0], helper * SHARD, SHARD, 0)
    points_shape = jax.ShapeDtypeStruct((SHARD, WIDTH), F32)
    level_shape = jax.ShapeDtypeStruct((8, SHARD), F32)
    named = None
    for _ in range(ITERS):
        targets, sources = from_blocks(copies, source)
        query = from_helpers(msg)
        if named is None:
            meta = jnp.concatenate([part[:, SHARD + META, :blocks] for part in targets])
            named = lax.dynamic_index_in_dim(meta, block, 1, False).astype(jnp.int32)
        parts = pl.pallas_call(
            attend_kernel,
            out_shape=jax.ShapeDtypeStruct((helpers, MSG, WIDTH), BF16),
            in_specs=[smem] * 5 + [vmem] * (XS + ZS + helpers),
            out_specs=vmem,
            scratch_shapes=[
                pltpu.SMEM((2, blocks + 1), jnp.int32),
                pltpu.VMEM((2 * blocks, SIDE, WIDTH), BF16),
                pltpu.VMEM((helpers * SHARD, WIDTH), BF16),
                pltpu.VMEM((helpers * SHARD, WIDTH), F32),
                pltpu.VMEM((helpers * SHARD, WIDTH), F32),
                pltpu.VMEM((helpers * SHARD, WIDTH), F32),
            ],
            name="attend",
        )(at, pairs, counts, owner, named, *targets, *sources, *query)
        got = exchanged(parts, HELP)
        tp, tl, sp, sl, msg, copies, source = pl.pallas_call(
            settle_kernel,
            out_shape=(
                points_shape, level_shape, points_shape, level_shape, msg_shape, copies_shape, source_shape
            ),
            in_specs=[vmem, vmem, vmem],
            out_specs=(vmem,) * 7,
            scratch_shapes=[pltpu.VMEM((WIDTH, SHARD), F32)],
            name="settle",
        )(got, tp, sp)
    done = gathered(jnp.concatenate([sp, sl], axis=0), HELP)
    new_source_points = done[:, :SHARD].reshape(1, helpers * SHARD, WIDTH)
    new_source_potential = done[:, SHARD].reshape(1, helpers * SHARD)
    return new_source_points, new_source_potential, tp[None], tl[:1]


def solution(mesh):
    torus = Mesh(mesh.devices.reshape(XS, ZS, YS, CS), ("x", "z", "y", "c"))
    blk = ("x", "z")
    in_specs = (
        P(blk, None, None),
        P(blk, None),
        P(blk, HELP, None),
        P(blk, HELP),
        P(blk, None),
        P(blk),
        P(),
    )
    out_specs = (P(blk, None, None), P(blk, None), P(blk, HELP, None), P(blk, HELP))
    return jax.shard_map(
        on_device, mesh=torus, in_specs=in_specs, out_specs=out_specs, check_vma=False
    )
```

```python
import functools

import jax
import jax.numpy as jnp
from jax import lax
from jax.experimental import pallas as pl
from jax.experimental.pallas import tpu as pltpu
from jax.sharding import Mesh
from jax.sharding import PartitionSpec as P

ITERS = 2
HELP = ("y", "c")
SHARD = 128
WIDTH = 128
SIDE = SHARD + 16
MSG = 2 * SIDE
META = 8
SQUARE = 9
LIMIT = 40.0
XS, ZS, YS, CS = 4, 8, 4, 2
TEMPER = 0.25
STRIDE = 0.5
LOW = -1e30

F32 = jnp.float32
BF16 = jnp.bfloat16
LANES = (((1,), (1,)), ((), ()))


def as_row(column):
    return jnp.broadcast_to(column, (SHARD, WIDTH)).T[:16]


def in_three(rows):
    hi = rows.astype(BF16)
    rest = rows - hi.astype(F32)
    mid = rest.astype(BF16)
    lo = (rest - mid.astype(F32)).astype(BF16)
    at = lax.broadcasted_iota(jnp.int32, rows.shape, 0)
    out = jnp.where(at == 0, hi.astype(F32), jnp.where(at == 1, mid.astype(F32), lo.astype(F32)))
    return jnp.where(at < 3, out, 0.0)


def of_three(rows):
    rows = rows.astype(F32)
    return rows[0:1] + rows[1:2] + rows[2:3]


def square_row(rounded):
    wide = rounded.astype(F32)
    return as_row(jnp.sum(wide * wide, axis=1, keepdims=True))


def write_side(msg_ref, copies_ref, source_ref, side, points, level_row, meta=None):
    rounded = points.astype(BF16)
    square = square_row(rounded)
    bias = level_row * (1.0 / TEMPER) - square * (1.0 / (WIDTH * TEMPER))
    at = lax.broadcasted_iota(jnp.int32, square.shape, 0)
    extras = jnp.where(at == SQUARE, square, in_three(bias))
    if meta is not None:
        extras = jnp.where(at == META, meta, extras)
    extras = extras.astype(BF16)
    msg_ref[pl.ds(side * SIDE, SHARD), :] = rounded
    msg_ref[pl.ds(side * SIDE + SHARD, 16), :] = extras
    if side == 0:
        for k in range(copies_ref.shape[0]):
            copies_ref[k, pl.ds(0, SHARD), :] = rounded
            copies_ref[k, pl.ds(SHARD, 16), :] = extras
    else:
        source_ref[pl.ds(0, SHARD), :] = rounded
        source_ref[pl.ds(SHARD, 16), :] = extras


def prepare_kernel(
    at_ref, pairs_ref, counts_ref, owner_ref, tp_ref, tl_ref, sp_ref, sl_ref, msg_ref, copies_ref, source_ref
):
    lane = lax.broadcasted_iota(jnp.int32, (1, WIDTH), 1)
    meta = jnp.zeros((1, WIDTH), F32)
    count = counts_ref[0]
    for slot in range(pairs_ref.shape[1]):
        partner = jnp.where(slot < count, owner_ref[pairs_ref[0, slot]], -1)
        meta = jnp.where(lane == partner, 1.0, meta)
    write_side(msg_ref, copies_ref, source_ref, 0, tp_ref[0], tl_ref[...], meta)
    write_side(msg_ref, copies_ref, source_ref, 1, sp_ref[0], sl_ref[...])


def attend_kernel(at_ref, pairs_ref, counts_ref, owner_ref, named_ref, *refs):
    far, ring, helpers = XS, ZS, YS * CS
    target_refs, refs = refs[:far], refs[far:]
    source_refs, refs = refs[:ring], refs[ring:]
    query_refs, refs = refs[:helpers], refs[helpers:]
    *out_refs, list_ref, key_ref, scaled_ref, shift_ref, sum_ref, acc_ref = refs
    at_x, at_z = at_ref[0], at_ref[1]
    blocks = far * ring
    for k in range(ring):
        key_ref[pl.ds(k * far, far)] = source_refs[k][...]
    for k in range(far):
        key_ref[pl.ds(blocks + k * ring, ring)] = target_refs[k][...]

    def largest(extras):
        top = functools.reduce(jnp.maximum, extras).astype(F32)
        return jnp.max(top[SQUARE : SQUARE + 1])

    bound = largest([key_ref[j, pl.ds(SHARD, 16), :] for j in range(2 * blocks)]) * largest(
        [ref[pl.ds(at, 16), :] for ref in query_refs for at in (SHARD, SIDE + SHARD)]
    )
    safe = bound * 1.03 <= (LIMIT * WIDTH * TEMPER / 2.0) ** 2

    def enlist_sources(j, count):
        list_ref[0, count] = ((at_z - j) & (ring - 1)) * far + j // ring
        return count + jnp.where(named_ref[j] > 0, 1, 0)

    def enlist_targets(s, carry):
        block = owner_ref[pairs_ref[0, s]]
        list_ref[1, s] = blocks + ((at_x - block // ring) & (far - 1)) * ring + (block & (ring - 1))
        return carry

    naming = lax.fori_loop(0, blocks, enlist_sources, 0)
    lax.fori_loop(0, pairs_ref.shape[1], enlist_targets, 0)

    def one_side(side, carry):
        q_at = pl.multiple_of(side * SIDE, 16)
        live = jnp.where(side == 0, naming, counts_ref[0])
        list_ref[side, live] = list_ref[side, 0]
        for c in range(helpers):
            scaled_ref[pl.ds(c * SHARD, SHARD), :] = query_refs[c][pl.ds(q_at, SHARD), :] * jnp.asarray(
                2.0 / (WIDTH * TEMPER), BF16
            )
        sum_ref[...] = jnp.zeros(sum_ref.shape, F32)
        acc_ref[...] = jnp.zeros(acc_ref.shape, F32)
        turns = (live + 1) // 2

        def biases(t):
            left = of_three(key_ref[list_ref[side, 2 * t], pl.ds(SHARD, 16), :])
            right = of_three(key_ref[list_ref[side, 2 * t + 1], pl.ds(SHARD, 16), :])
            return left, jnp.where(2 * t + 1 < live, right, LOW)

        def scores(t, shift, rows):
            first = key_ref[list_ref[side, 2 * t], pl.ds(0, SHARD), :]
            second = key_ref[list_ref[side, 2 * t + 1], pl.ds(0, SHARD), :]
            key = jnp.concatenate([first, second], axis=0)
            left, right = biases(t)
            cross = lax.dot_general(scaled_ref[rows, :], key, LANES, preferred_element_type=F32)
            return cross[:, :SHARD] + (left - shift), cross[:, SHARD:] + (right - shift), key

        def add(left, right, key, rows):
            left = jnp.exp(left)
            right = jnp.exp(right)
            sum_ref[rows, :] += left + right
            weight = jnp.concatenate([left.astype(BF16), right.astype(BF16)], axis=1)
            acc_ref[rows, :] += jnp.dot(weight, key, preferred_element_type=F32)

        @pl.when(safe)
        def _():
            def top_bias(t, top):
                left, right = biases(t)
                return jnp.maximum(top, jnp.maximum(left, right))

            top = lax.fori_loop(0, turns, top_bias, jnp.full((1, WIDTH), LOW, F32))
            top = jnp.max(top, axis=1, keepdims=True)
            shift_ref[...] = jnp.broadcast_to(top, shift_ref.shape)

            def add_up(t, carry):
                rows = pl.ds(0, helpers * SHARD)
                add(*scores(t, top, rows), rows)
                return carry

            lax.fori_loop(0, turns, add_up, 0)

        @pl.when(jnp.logical_not(safe))
        def _():
            def one_part(c, carry):
                rows = pl.ds(pl.multiple_of(c * SHARD, SHARD), SHARD)

                def find_peak(t, peak):
                    left, right, _ = scores(t, 0.0, rows)
                    return jnp.maximum(peak, jnp.maximum(left, right))

                peak = lax.fori_loop(0, turns, find_peak, jnp.full((SHARD, WIDTH), LOW, F32))
                top = jnp.broadcast_to(jnp.max(peak, axis=1, keepdims=True), (SHARD, WIDTH))
                shift_ref[:, rows] = top.T[:16]

                def add_up(t, carry):
                    left, right, key = scores(t, 0.0, rows)
                    add(left - top, right - top, key, rows)
                    return carry

                return lax.fori_loop(0, turns, add_up, carry)

            lax.fori_loop(0, helpers, one_part, 0)

        whole = sum_ref[...]
        hi = whole.astype(BF16)
        mid = (whole - hi.astype(F32)).astype(BF16)
        ones = jnp.ones((WIDTH, WIDTH), BF16)
        across = jnp.dot(hi, ones, preferred_element_type=F32) + jnp.dot(mid, ones, preferred_element_type=F32)
        mean = (acc_ref[...] * (1.0 / across)).astype(BF16)
        few = jnp.ones((16, WIDTH), BF16)
        total = lax.dot_general(few, hi, LANES, preferred_element_type=F32)
        total += lax.dot_general(few, mid, LANES, preferred_element_type=F32)
        lse = in_three(shift_ref[...] + jnp.log(total)).astype(BF16)
        for c in range(helpers):
            rows = slice(c * SHARD, (c + 1) * SHARD)
            out_ref, to = out_refs[c % CS], -(c // CS) % YS
            out_ref[to, pl.ds(q_at, SHARD), :] = mean[rows]
            out_ref[to, pl.ds(pl.multiple_of(q_at + SHARD, 16), 16), :] = lse[:, rows]
        return carry

    lax.fori_loop(0, 2, one_side, 0)


def merge_kernel(own_ref, other_ref, *refs):
    *out_refs, scr_ref = refs
    cases = [(k, side * SIDE) for k in range(len(out_refs)) for side in range(2)]
    scr_ref[...] = jnp.zeros(scr_ref.shape, F32)
    for n, (k, at) in enumerate(cases):
        own = of_three(own_ref[k, pl.ds(at + SHARD, 16), :])
        other = of_three(other_ref[k, pl.ds(at + SHARD, 16), :])
        top = jnp.maximum(own, other)
        share = jnp.exp(own - top)
        total = share + jnp.exp(other - top)
        scr_ref[pl.ds(n, 1), :] = share / total
        lse = jnp.broadcast_to(top + jnp.log(total), (16, SHARD))
        out_refs[k][pl.ds(at + SHARD, 16), :] = in_three(lse).astype(BF16)
    columns = scr_ref[...].T
    for n, (k, at) in enumerate(cases):
        own = own_ref[k, pl.ds(at, SHARD), :].astype(F32)
        other = other_ref[k, pl.ds(at, SHARD), :].astype(F32)
        out_refs[k][pl.ds(at, SHARD), :] = (other + columns[:, n : n + 1] * (own - other)).astype(BF16)


def settle_kernel(*refs):
    got_refs, refs = refs[:YS], refs[YS:]
    tp_ref, sp_ref, ntp_ref, ntl_ref, nsp_ref, nsl_ref, msg_ref, copies_ref, source_ref, scr_ref = refs
    sides = ((0, tp_ref, ntp_ref, ntl_ref), (1, sp_ref, nsp_ref, nsl_ref))
    for side, old_ref, new_ref, level_ref in sides:
        at = side * SIDE
        parts = [of_three(ref[pl.ds(at + SHARD, 16), :]) for ref in got_refs]
        top = functools.reduce(jnp.maximum, parts)
        shares = [jnp.exp(part - top) for part in parts]
        total = functools.reduce(jnp.add, shares)
        scr_ref[...] = jnp.zeros(scr_ref.shape, F32)
        for h, share in enumerate(shares):
            scr_ref[pl.ds(h, 1), :] = share / total
        columns = scr_ref[...].T
        mean = jnp.zeros((SHARD, WIDTH), F32)
        for h, ref in enumerate(got_refs):
            mean = mean + columns[:, h : h + 1] * ref[pl.ds(at, SHARD), :].astype(F32)
        old = old_ref[pl.ds(0, SHARD), :]
        square = square_row(old.astype(BF16))
        level = -TEMPER * (top + jnp.log(total) - square * (1.0 / (WIDTH * TEMPER)))
        new = old + STRIDE * (mean - old)
        new_ref[pl.ds(0, SHARD), :] = new
        level_ref[...] = level[:8]
        if side:
            new_ref[pl.ds(SHARD, 8), :] = level[:8]
        write_side(msg_ref, copies_ref, source_ref, side, new, level)


def finish_kernel(at_ref, *refs):
    *piece_refs, points_ref, level_ref = refs
    for n, ref in enumerate(piece_refs):
        helper = ((at_ref[2] - n // CS) & (YS - 1)) * CS + ((at_ref[3] + n) & (CS - 1))
        points_ref[0, pl.ds(pl.multiple_of(helper * SHARD, SHARD), SHARD), :] = ref[pl.ds(0, SHARD), :]
        level_ref[pl.ds(helper, 1), :] = ref[pl.ds(SHARD, 1), :]


def exchanged(copies, axes):
    return lax.all_to_all(copies, axes, split_axis=0, concat_axis=0, tiled=True)


def shifted(x, axis, step):
    n = lax.axis_size(axis)
    return lax.ppermute(x, axis, [(i, (i + step) % n) for i in range(n)])


def from_helpers(msg):
    pieces = []
    for k in range(YS):
        piece = shifted(msg, "y", k) if k else msg
        pieces += [piece, shifted(piece, "c", 1)]
    return pieces


def from_blocks(copies, source):
    sides = [source] + [shifted(source, "x", k) for k in range(1, XS)]
    near = exchanged(copies, "z")
    ring = [None] * ZS
    ring[0] = ahead = back = jnp.stack(sides)
    targets = [near]
    for k in range(1, XS):
        targets.append(shifted(near, "x", k))
    for k in range(1, ZS // 2 + 1):
        ring[k] = ahead = shifted(ahead, "z", 1)
        if k < ZS // 2:
            ring[ZS - k] = back = shifted(back, "z", ZS - 1)
    return targets, ring


def on_device(
    source_points, source_potential, target_points, target_potential, pairs, counts, owner
):
    helper = lax.axis_index(HELP)
    block = lax.axis_index(("x", "z"))
    blocks = XS * ZS
    helpers = YS * CS
    at = jnp.stack([lax.axis_index(axis) for axis in ("x", "z", "y", "c")])
    smem = pl.BlockSpec(memory_space=pltpu.SMEM)
    vmem = pl.BlockSpec(memory_space=pltpu.VMEM)
    msg_shape = jax.ShapeDtypeStruct((MSG, WIDTH), BF16)
    copies_shape = jax.ShapeDtypeStruct((ZS, SIDE, WIDTH), BF16)
    source_shape = jax.ShapeDtypeStruct((SIDE, WIDTH), BF16)
    half_shape = jax.ShapeDtypeStruct((YS, MSG, WIDTH), BF16)
    final_shape = jax.ShapeDtypeStruct((SHARD + 8, WIDTH), F32)
    own_points = pl.BlockSpec((1, SHARD, WIDTH), lambda i, at: (0, at[2] * CS + at[3], 0))
    own_level = pl.BlockSpec((1, SHARD), lambda i, at: (0, at[2] * CS + at[3]))
    whole = lambda *shape: pl.BlockSpec(shape, lambda i, at: (0,) * len(shape))
    msg, copies, source = pl.pallas_call(
        prepare_kernel,
        out_shape=(msg_shape, copies_shape, source_shape),
        grid_spec=pltpu.PrefetchScalarGridSpec(
            num_scalar_prefetch=1,
            grid=(1,),
            in_specs=[smem, smem, smem, whole(1, SHARD, WIDTH), whole(1, SHARD), own_points, own_level],
            out_specs=(whole(*msg_shape.shape), whole(*copies_shape.shape), whole(*source_shape.shape)),
        ),
        name="prepare",
    )(at, pairs, counts, owner, target_points, target_potential, source_points, source_potential)
    tp = target_points[0]
    sp = lax.dynamic_slice_in_dim(source_points[0], helper * SHARD, SHARD, 0)
    points_shape = jax.ShapeDtypeStruct((SHARD, WIDTH), F32)
    level_shape = jax.ShapeDtypeStruct((8, SHARD), F32)
    named = None
    for _ in range(ITERS):
        targets, sources = from_blocks(copies, source)
        query = from_helpers(msg)
        if named is None:
            meta = jnp.concatenate([part[:, SHARD + META, :blocks] for part in targets])
            named = lax.dynamic_index_in_dim(meta, block, 1, False).astype(jnp.int32)
        own, other = pl.pallas_call(
            attend_kernel,
            out_shape=(half_shape, half_shape),
            in_specs=[smem] * 5 + [vmem] * (XS + ZS + helpers),
            out_specs=(vmem, vmem),
            scratch_shapes=[
                pltpu.SMEM((2, blocks + 1), jnp.int32),
                pltpu.VMEM((2 * blocks, SIDE, WIDTH), BF16),
                pltpu.VMEM((helpers * SHARD, WIDTH), BF16),
                pltpu.VMEM((16, helpers * SHARD), F32),
                pltpu.VMEM((helpers * SHARD, WIDTH), F32),
                pltpu.VMEM((helpers * SHARD, WIDTH), F32),
            ],
            name="attend",
        )(at, pairs, counts, owner, named, *targets, *sources, *query)
        other = shifted(other, "c", 1)
        merged = pl.pallas_call(
            merge_kernel,
            out_shape=(msg_shape,) * YS,
            in_specs=[vmem, vmem],
            out_specs=(vmem,) * YS,
            scratch_shapes=[pltpu.VMEM((WIDTH, SHARD), F32)],
            name="merge",
        )(own, other)
        got = [shifted(part, "y", k) if k else part for k, part in enumerate(merged)]
        tp, tl, sp, _, msg, copies, source = pl.pallas_call(
            settle_kernel,
            out_shape=(
                points_shape, level_shape, final_shape, level_shape, msg_shape, copies_shape, source_shape
            ),
            in_specs=[vmem] * (YS + 2),
            out_specs=(vmem,) * 7,
            scratch_shapes=[pltpu.VMEM((WIDTH, SHARD), F32)],
            name="settle",
        )(*got, tp, sp)
    new_source_points, new_source_potential = pl.pallas_call(
        finish_kernel,
        out_shape=(jax.ShapeDtypeStruct(source_points.shape, F32), jax.ShapeDtypeStruct((helpers, SHARD), F32)),
        in_specs=[smem] + [vmem] * helpers,
        out_specs=(vmem, vmem),
        name="finish",
    )(at, *from_helpers(sp))
    return new_source_points, new_source_potential.reshape(source_potential.shape), tp[None], tl[:1]


def solution(mesh):
    torus = Mesh(mesh.devices.reshape(XS, ZS, YS, CS), ("x", "z", "y", "c"))
    blk = ("x", "z")
    in_specs = (
        P(blk, None, None),
        P(blk, None),
        P(blk, HELP, None),
        P(blk, HELP),
        P(blk, None),
        P(blk),
        P(),
    )
    out_specs = (P(blk, None, None), P(blk, None), P(blk, HELP, None), P(blk, HELP))
    return jax.shard_map(
        on_device, mesh=torus, in_specs=in_specs, out_specs=out_specs, check_vma=False
    )
```

```python
import functools

import jax
import jax.numpy as jnp
from jax import lax
from jax.experimental import pallas as pl
from jax.experimental.pallas import tpu as pltpu
from jax.sharding import Mesh
from jax.sharding import PartitionSpec as P

ITERS = 2
HELP = ("y", "c")
SHARD = 128
WIDTH = 128
SIDE = SHARD + 16
MSG = 2 * SIDE
META = 8
SQUARE = 9
LIMIT = 40.0
XS, ZS, YS, CS = 4, 8, 4, 2
TEMPER = 0.25
STRIDE = 0.5
LOW = -1e30

F32 = jnp.float32
BF16 = jnp.bfloat16
LANES = (((1,), (1,)), ((), ()))


def as_row(column):
    return jnp.broadcast_to(column, (SHARD, WIDTH)).T[:16]


def in_three(rows):
    hi = rows.astype(BF16)
    rest = rows - hi.astype(F32)
    mid = rest.astype(BF16)
    lo = (rest - mid.astype(F32)).astype(BF16)
    at = lax.broadcasted_iota(jnp.int32, rows.shape, 0)
    out = jnp.where(at == 0, hi.astype(F32), jnp.where(at == 1, mid.astype(F32), lo.astype(F32)))
    return jnp.where(at < 3, out, 0.0)


def of_three(rows):
    rows = rows.astype(F32)
    return rows[0:1] + rows[1:2] + rows[2:3]


def square_row(rounded):
    wide = rounded.astype(F32)
    return as_row(jnp.sum(wide * wide, axis=1, keepdims=True))


def write_side(msg_ref, copies_ref, source_ref, side, points, level_row, meta=None):
    rounded = points.astype(BF16)
    square = square_row(rounded)
    bias = level_row * (1.0 / TEMPER) - square * (1.0 / (WIDTH * TEMPER))
    at = lax.broadcasted_iota(jnp.int32, square.shape, 0)
    extras = jnp.where(at == SQUARE, square, in_three(bias))
    if meta is not None:
        extras = jnp.where(at == META, meta, extras)
    extras = extras.astype(BF16)
    msg_ref[pl.ds(side * SIDE, SHARD), :] = rounded
    msg_ref[pl.ds(side * SIDE + SHARD, 16), :] = extras
    if side == 0:
        for k in range(copies_ref.shape[0]):
            copies_ref[k, pl.ds(0, SHARD), :] = rounded
            copies_ref[k, pl.ds(SHARD, 16), :] = extras
    else:
        source_ref[pl.ds(0, SHARD), :] = rounded
        source_ref[pl.ds(SHARD, 16), :] = extras


def prepare_kernel(
    at_ref, pairs_ref, counts_ref, owner_ref, tp_ref, tl_ref, sp_ref, sl_ref, msg_ref, copies_ref, source_ref
):
    lane = lax.broadcasted_iota(jnp.int32, (1, WIDTH), 1)
    meta = jnp.zeros((1, WIDTH), F32)
    count = counts_ref[0]
    for slot in range(pairs_ref.shape[1]):
        partner = jnp.where(slot < count, owner_ref[pairs_ref[0, slot]], -1)
        meta = jnp.where(lane == partner, 1.0, meta)
    write_side(msg_ref, copies_ref, source_ref, 0, tp_ref[0], tl_ref[...], meta)
    write_side(msg_ref, copies_ref, source_ref, 1, sp_ref[0], sl_ref[...])


def attend_kernel(at_ref, pairs_ref, counts_ref, owner_ref, named_ref, *refs):
    far, ring, helpers = XS, ZS, YS * CS
    target_refs, refs = refs[:far], refs[far:]
    source_refs, refs = refs[:ring], refs[ring:]
    query_refs, refs = [ref.at[n] for ref in refs[:YS] for n in range(CS)], refs[YS:]
    *out_refs, list_ref, key_ref, scaled_ref, shift_ref, sum_ref, acc_ref = refs
    at_x, at_z = at_ref[0], at_ref[1]
    blocks = far * ring
    for k in range(ring):
        key_ref[pl.ds(k * far, far)] = source_refs[k][...]
    for k in range(far):
        key_ref[pl.ds(blocks + k * ring, ring)] = target_refs[k][...]

    def largest(extras):
        top = functools.reduce(jnp.maximum, extras).astype(F32)
        return jnp.max(top[SQUARE : SQUARE + 1])

    bound = largest([key_ref[j, pl.ds(SHARD, 16), :] for j in range(2 * blocks)]) * largest(
        [ref[pl.ds(at, 16), :] for ref in query_refs for at in (SHARD, SIDE + SHARD)]
    )
    safe = bound * 1.03 <= (LIMIT * WIDTH * TEMPER / 2.0) ** 2

    def enlist_sources(j, count):
        list_ref[0, count] = ((at_z - j) & (ring - 1)) * far + j // ring
        return count + jnp.where(named_ref[j] > 0, 1, 0)

    def enlist_targets(s, carry):
        block = owner_ref[pairs_ref[0, s]]
        list_ref[1, s] = blocks + ((at_x - block // ring) & (far - 1)) * ring + (block & (ring - 1))
        return carry

    naming = lax.fori_loop(0, blocks, enlist_sources, 0)
    lax.fori_loop(0, pairs_ref.shape[1], enlist_targets, 0)

    def one_side(side, carry):
        q_at = pl.multiple_of(side * SIDE, 16)
        live = jnp.where(side == 0, naming, counts_ref[0])
        list_ref[side, live] = list_ref[side, 0]
        for c in range(helpers):
            scaled_ref[pl.ds(c * SHARD, SHARD), :] = query_refs[c][pl.ds(q_at, SHARD), :] * jnp.asarray(
                2.0 / (WIDTH * TEMPER), BF16
            )
        sum_ref[...] = jnp.zeros(sum_ref.shape, F32)
        acc_ref[...] = jnp.zeros(acc_ref.shape, F32)
        turns = (live + 1) // 2

        def biases(t):
            left = of_three(key_ref[list_ref[side, 2 * t], pl.ds(SHARD, 16), :])
            right = of_three(key_ref[list_ref[side, 2 * t + 1], pl.ds(SHARD, 16), :])
            return left, jnp.where(2 * t + 1 < live, right, LOW)

        def scores(t, shift, rows):
            first = key_ref[list_ref[side, 2 * t], pl.ds(0, SHARD), :]
            second = key_ref[list_ref[side, 2 * t + 1], pl.ds(0, SHARD), :]
            key = jnp.concatenate([first, second], axis=0)
            left, right = biases(t)
            cross = lax.dot_general(scaled_ref[rows, :], key, LANES, preferred_element_type=F32)
            return cross[:, :SHARD] + (left - shift), cross[:, SHARD:] + (right - shift), key

        def add(left, right, key, rows):
            left = jnp.exp(left)
            right = jnp.exp(right)
            sum_ref[rows, :] += left + right
            weight = jnp.concatenate([left.astype(BF16), right.astype(BF16)], axis=1)
            acc_ref[rows, :] += jnp.dot(weight, key, preferred_element_type=F32)

        @pl.when(safe)
        def _():
            def top_bias(t, top):
                left, right = biases(t)
                return jnp.maximum(top, jnp.maximum(left, right))

            top = lax.fori_loop(0, turns, top_bias, jnp.full((1, WIDTH), LOW, F32))
            top = jnp.max(top, axis=1, keepdims=True)
            shift_ref[...] = jnp.broadcast_to(top, shift_ref.shape)

            def add_up(t, carry):
                rows = pl.ds(0, helpers * SHARD)
                add(*scores(t, top, rows), rows)
                return carry

            lax.fori_loop(0, turns, add_up, 0)

        @pl.when(jnp.logical_not(safe))
        def _():
            def one_part(c, carry):
                rows = pl.ds(pl.multiple_of(c * SHARD, SHARD), SHARD)

                def find_peak(t, peak):
                    left, right, _ = scores(t, 0.0, rows)
                    return jnp.maximum(peak, jnp.maximum(left, right))

                peak = lax.fori_loop(0, turns, find_peak, jnp.full((SHARD, WIDTH), LOW, F32))
                top = jnp.broadcast_to(jnp.max(peak, axis=1, keepdims=True), (SHARD, WIDTH))
                shift_ref[:, rows] = top.T[:16]

                def add_up(t, carry):
                    left, right, key = scores(t, 0.0, rows)
                    add(left - top, right - top, key, rows)
                    return carry

                return lax.fori_loop(0, turns, add_up, carry)

            lax.fori_loop(0, helpers, one_part, 0)

        whole = sum_ref[...]
        hi = whole.astype(BF16)
        mid = (whole - hi.astype(F32)).astype(BF16)
        ones = jnp.ones((WIDTH, WIDTH), BF16)
        across = jnp.dot(hi, ones, preferred_element_type=F32) + jnp.dot(mid, ones, preferred_element_type=F32)
        mean = (acc_ref[...] * (1.0 / across)).astype(BF16)
        few = jnp.ones((16, WIDTH), BF16)
        total = lax.dot_general(few, hi, LANES, preferred_element_type=F32)
        total += lax.dot_general(few, mid, LANES, preferred_element_type=F32)
        lse = in_three(shift_ref[...] + jnp.log(total)).astype(BF16)
        for c in range(helpers):
            rows = slice(c * SHARD, (c + 1) * SHARD)
            out_ref, to = out_refs[c % CS], -(c // CS) % YS
            out_ref[to, pl.ds(q_at, SHARD), :] = mean[rows]
            out_ref[to, pl.ds(pl.multiple_of(q_at + SHARD, 16), 16), :] = lse[:, rows]
        return carry

    lax.fori_loop(0, 2, one_side, 0)


def merge_kernel(own_ref, other_ref, *refs):
    *out_refs, scr_ref = refs
    cases = [(k, side * SIDE) for k in range(len(out_refs)) for side in range(2)]
    scr_ref[...] = jnp.zeros(scr_ref.shape, F32)
    for n, (k, at) in enumerate(cases):
        own = of_three(own_ref[k, pl.ds(at + SHARD, 16), :])
        other = of_three(other_ref[k, pl.ds(at + SHARD, 16), :])
        top = jnp.maximum(own, other)
        share = jnp.exp(own - top)
        total = share + jnp.exp(other - top)
        scr_ref[pl.ds(n, 1), :] = share / total
        lse = jnp.broadcast_to(top + jnp.log(total), (16, SHARD))
        out_refs[k][pl.ds(at + SHARD, 16), :] = in_three(lse).astype(BF16)
    columns = scr_ref[...].T
    for n, (k, at) in enumerate(cases):
        own = own_ref[k, pl.ds(at, SHARD), :].astype(F32)
        other = other_ref[k, pl.ds(at, SHARD), :].astype(F32)
        out_refs[k][pl.ds(at, SHARD), :] = (other + columns[:, n : n + 1] * (own - other)).astype(BF16)


def settle_kernel(*refs):
    got_refs, refs = refs[:YS], refs[YS:]
    tp_ref, sp_ref, ntp_ref, ntl_ref, nsp_ref, nsl_ref, msg_ref, copies_ref, source_ref, scr_ref = refs
    sides = ((0, tp_ref, ntp_ref, ntl_ref), (1, sp_ref, nsp_ref, nsl_ref))
    for side, old_ref, new_ref, level_ref in sides:
        at = side * SIDE
        parts = [of_three(ref[pl.ds(at + SHARD, 16), :]) for ref in got_refs]
        top = functools.reduce(jnp.maximum, parts)
        shares = [jnp.exp(part - top) for part in parts]
        total = functools.reduce(jnp.add, shares)
        scr_ref[...] = jnp.zeros(scr_ref.shape, F32)
        for h, share in enumerate(shares):
            scr_ref[pl.ds(h, 1), :] = share / total
        columns = scr_ref[...].T
        mean = jnp.zeros((SHARD, WIDTH), F32)
        for h, ref in enumerate(got_refs):
            mean = mean + columns[:, h : h + 1] * ref[pl.ds(at, SHARD), :].astype(F32)
        old = old_ref[pl.ds(0, SHARD), :]
        square = square_row(old.astype(BF16))
        level = -TEMPER * (top + jnp.log(total) - square * (1.0 / (WIDTH * TEMPER)))
        new = old + STRIDE * (mean - old)
        new_ref[pl.ds(0, SHARD), :] = new
        level_ref[...] = level[:8]
        if side:
            new_ref[pl.ds(SHARD, 8), :] = level[:8]
        write_side(msg_ref, copies_ref, source_ref, side, new, level)


def finish_kernel(at_ref, *refs):
    own_ref, other_ref, points_ref, level_ref = refs
    for n in range(YS * CS):
        ref = (own_ref, other_ref)[n % CS].at[n // CS]
        helper = ((at_ref[2] - n // CS) & (YS - 1)) * CS + ((at_ref[3] + n) & (CS - 1))
        points_ref[0, pl.ds(pl.multiple_of(helper * SHARD, SHARD), SHARD), :] = ref[pl.ds(0, SHARD), :]
        level_ref[pl.ds(helper, 1), :] = ref[pl.ds(SHARD, 1), :]


def near_core(*arrays):
    return [pltpu.with_memory_space_constraint(x, pltpu.VMEM) for x in arrays]


def exchanged(copies, axes):
    return lax.all_to_all(copies, axes, split_axis=0, concat_axis=0, tiled=True)


def shifted(x, axis, step):
    n = lax.axis_size(axis)
    return lax.ppermute(x, axis, [(i, (i + step) % n) for i in range(n)])


def from_helpers(msg):
    pair = jnp.stack([msg, shifted(msg, "c", 1)])
    return [shifted(pair, "y", k) if k else pair for k in range(YS)]


def from_helpers_late(msg):
    own = jnp.stack([shifted(msg, "y", k) if k else msg for k in range(YS)])
    return own, shifted(own, "c", 1)


def from_blocks(copies, source):
    sides = [source] + [shifted(source, "x", k) for k in range(1, XS)]
    near = exchanged(copies, "z")
    ring = [None] * ZS
    ring[0] = ahead = back = jnp.stack(sides)
    targets = [near]
    for k in range(1, XS):
        targets.append(shifted(near, "x", k))
    for k in range(1, ZS // 2 + 1):
        ring[k] = ahead = shifted(ahead, "z", 1)
        if k < ZS // 2:
            ring[ZS - k] = back = shifted(back, "z", ZS - 1)
    return targets, ring


def on_device(
    source_points, source_potential, target_points, target_potential, pairs, counts, owner
):
    helper = lax.axis_index(HELP)
    block = lax.axis_index(("x", "z"))
    blocks = XS * ZS
    helpers = YS * CS
    at = jnp.stack([lax.axis_index(axis) for axis in ("x", "z", "y", "c")])
    smem = pl.BlockSpec(memory_space=pltpu.SMEM)
    vmem = pl.BlockSpec(memory_space=pltpu.VMEM)
    msg_shape = pltpu.VMEM((MSG, WIDTH), BF16)
    copies_shape = pltpu.VMEM((ZS, SIDE, WIDTH), BF16)
    source_shape = pltpu.VMEM((SIDE, WIDTH), BF16)
    half_shape = pltpu.VMEM((YS, MSG, WIDTH), BF16)
    final_shape = pltpu.VMEM((SHARD + 8, WIDTH), F32)
    own_points = pl.BlockSpec((1, SHARD, WIDTH), lambda i, at: (0, at[2] * CS + at[3], 0))
    own_level = pl.BlockSpec((1, SHARD), lambda i, at: (0, at[2] * CS + at[3]))
    whole = lambda *shape: pl.BlockSpec(shape, lambda i, at: (0,) * len(shape))
    msg, copies, source = pl.pallas_call(
        prepare_kernel,
        out_shape=(msg_shape, copies_shape, source_shape),
        grid_spec=pltpu.PrefetchScalarGridSpec(
            num_scalar_prefetch=1,
            grid=(1,),
            in_specs=[smem, smem, smem, whole(1, SHARD, WIDTH), whole(1, SHARD), own_points, own_level],
            out_specs=(whole(*msg_shape.shape), whole(*copies_shape.shape), whole(*source_shape.shape)),
        ),
        name="prepare",
    )(at, pairs, counts, owner, target_points, target_potential, source_points, source_potential)
    tp = target_points[0]
    sp = lax.dynamic_slice_in_dim(source_points[0], helper * SHARD, SHARD, 0)
    points_shape = jax.ShapeDtypeStruct((SHARD, WIDTH), F32)
    level_shape = jax.ShapeDtypeStruct((8, SHARD), F32)
    named = None
    for _ in range(ITERS):
        targets, sources = from_blocks(copies, source)
        query = from_helpers(msg)
        if named is None:
            meta = jnp.concatenate([part[:, SHARD + META, :blocks] for part in targets])
            named = lax.dynamic_index_in_dim(meta, block, 1, False).astype(jnp.int32)
        own, other = pl.pallas_call(
            attend_kernel,
            out_shape=(half_shape, half_shape),
            in_specs=[smem] * 5 + [vmem] * (XS + ZS + YS),
            out_specs=(vmem, vmem),
            scratch_shapes=[
                pltpu.SMEM((2, blocks + 1), jnp.int32),
                pltpu.VMEM((2 * blocks, SIDE, WIDTH), BF16),
                pltpu.VMEM((helpers * SHARD, WIDTH), BF16),
                pltpu.VMEM((16, helpers * SHARD), F32),
                pltpu.VMEM((helpers * SHARD, WIDTH), F32),
                pltpu.VMEM((helpers * SHARD, WIDTH), F32),
            ],
            name="attend",
        )(at, pairs, counts, owner, named, *targets, *sources, *query)
        other = shifted(other, "c", 1)
        merged = pl.pallas_call(
            merge_kernel,
            out_shape=(msg_shape,) * YS,
            in_specs=[vmem, vmem],
            out_specs=(vmem,) * YS,
            scratch_shapes=[pltpu.VMEM((WIDTH, SHARD), F32)],
            name="merge",
        )(*near_core(own, other))
        got = [shifted(part, "y", k) if k else part for k, part in enumerate(merged)]
        tp, tl, sp, _, msg, copies, source = pl.pallas_call(
            settle_kernel,
            out_shape=(
                points_shape, level_shape, final_shape, level_shape, msg_shape, copies_shape, source_shape
            ),
            in_specs=[vmem] * (YS + 2),
            out_specs=(vmem,) * 7,
            scratch_shapes=[pltpu.VMEM((WIDTH, SHARD), F32)],
            name="settle",
        )(*near_core(*got), tp, sp)
    new_source_points, new_source_potential = pl.pallas_call(
        finish_kernel,
        out_shape=(jax.ShapeDtypeStruct(source_points.shape, F32), jax.ShapeDtypeStruct((helpers, SHARD), F32)),
        in_specs=[smem, vmem, vmem],
        out_specs=(vmem, vmem),
        name="finish",
    )(at, *near_core(*from_helpers_late(sp)))
    return new_source_points, new_source_potential.reshape(source_potential.shape), tp[None], tl[:1]


def solution(mesh):
    torus = Mesh(mesh.devices.reshape(XS, ZS, YS, CS), ("x", "z", "y", "c"))
    blk = ("x", "z")
    in_specs = (
        P(blk, None, None),
        P(blk, None),
        P(blk, HELP, None),
        P(blk, HELP),
        P(blk, None),
        P(blk),
        P(),
    )
    out_specs = (P(blk, None, None), P(blk, None), P(blk, HELP, None), P(blk, HELP))
    return jax.shard_map(
        on_device, mesh=torus, in_specs=in_specs, out_specs=out_specs, check_vma=False
    )
```

```python
import functools

import jax
import jax.numpy as jnp
from jax import lax
from jax.experimental import pallas as pl
from jax.experimental.pallas import tpu as pltpu
from jax.sharding import Mesh
from jax.sharding import PartitionSpec as P

ITERS = 2
HELP = ("y", "c")
SHARD = 128
WIDTH = 128
SIDE = SHARD + 16
MSG = 2 * SIDE
META = 8
SQUARE = 9
LIMIT = 40.0
XS, ZS, YS, CS = 4, 8, 4, 2
TEMPER = 0.25
STRIDE = 0.5
LOW = -1e30

F32 = jnp.float32
BF16 = jnp.bfloat16
LANES = (((1,), (1,)), ((), ()))


def as_row(column):
    return jnp.broadcast_to(column, (SHARD, WIDTH)).T[:16]


def in_three(rows):
    hi = rows.astype(BF16)
    rest = rows - hi.astype(F32)
    mid = rest.astype(BF16)
    lo = (rest - mid.astype(F32)).astype(BF16)
    at = lax.broadcasted_iota(jnp.int32, rows.shape, 0)
    out = jnp.where(at == 0, hi.astype(F32), jnp.where(at == 1, mid.astype(F32), lo.astype(F32)))
    return jnp.where(at < 3, out, 0.0)


def of_three(rows):
    rows = rows.astype(F32)
    return rows[0:1] + rows[1:2] + rows[2:3]


def square_row(rounded):
    wide = rounded.astype(F32)
    return as_row(jnp.sum(wide * wide, axis=1, keepdims=True))


def write_side(msg_ref, copies_ref, source_ref, side, points, level_row, meta=None):
    rounded = points.astype(BF16)
    square = square_row(rounded)
    bias = level_row * (1.0 / TEMPER) - square * (1.0 / (WIDTH * TEMPER))
    at = lax.broadcasted_iota(jnp.int32, square.shape, 0)
    extras = jnp.where(at == SQUARE, square, in_three(bias))
    if meta is not None:
        extras = jnp.where(at == META, meta, extras)
    extras = extras.astype(BF16)
    msg_ref[pl.ds(side * SIDE, SHARD), :] = rounded
    msg_ref[pl.ds(side * SIDE + SHARD, 16), :] = extras
    if side == 0:
        for k in range(copies_ref.shape[0]):
            copies_ref[k, pl.ds(0, SHARD), :] = rounded
            copies_ref[k, pl.ds(SHARD, 16), :] = extras
    else:
        source_ref[pl.ds(0, SHARD), :] = rounded
        source_ref[pl.ds(SHARD, 16), :] = extras


def prepare_kernel(
    at_ref, pairs_ref, counts_ref, owner_ref, tp_ref, tl_ref, sp_ref, sl_ref, msg_ref, copies_ref, source_ref
):
    lane = lax.broadcasted_iota(jnp.int32, (1, WIDTH), 1)
    meta = jnp.zeros((1, WIDTH), F32)
    count = counts_ref[0]
    for slot in range(pairs_ref.shape[1]):
        partner = jnp.where(slot < count, owner_ref[pairs_ref[0, slot]], -1)
        meta = jnp.where(lane == partner, 1.0, meta)
    write_side(msg_ref, copies_ref, source_ref, 0, tp_ref[0], tl_ref[...], meta)
    write_side(msg_ref, copies_ref, source_ref, 1, sp_ref[0], sl_ref[...])


def attend_kernel(at_ref, pairs_ref, counts_ref, owner_ref, named_ref, *refs):
    far, ring, helpers = XS, ZS, YS * CS
    target_refs, refs = refs[:far], refs[far:]
    source_refs, refs = refs[:ring], refs[ring:]
    query_refs, refs = [ref.at[n] for ref in refs[:YS] for n in range(CS)], refs[YS:]
    *out_refs, list_ref, key_ref, scaled_ref, shift_ref, sum_ref, acc_ref = refs
    at_x, at_z = at_ref[0], at_ref[1]
    blocks = far * ring
    for k in range(ring):
        key_ref[pl.ds(k * far, far)] = source_refs[k][...]
    for k in range(far):
        key_ref[pl.ds(blocks + k * ring, ring)] = target_refs[k][...]

    def largest(extras):
        top = functools.reduce(jnp.maximum, extras).astype(F32)
        return jnp.max(top[SQUARE : SQUARE + 1])

    bound = largest([key_ref[j, pl.ds(SHARD, 16), :] for j in range(2 * blocks)]) * largest(
        [ref[pl.ds(at, 16), :] for ref in query_refs for at in (SHARD, SIDE + SHARD)]
    )
    safe = bound * 1.03 <= (LIMIT * WIDTH * TEMPER / 2.0) ** 2

    def enlist_sources(j, count):
        list_ref[0, count] = ((at_z - j) & (ring - 1)) * far + j // ring
        return count + jnp.where(named_ref[j] > 0, 1, 0)

    def enlist_targets(s, carry):
        block = owner_ref[pairs_ref[0, s]]
        list_ref[1, s] = blocks + ((at_x - block // ring) & (far - 1)) * ring + (block & (ring - 1))
        return carry

    naming = lax.fori_loop(0, blocks, enlist_sources, 0)
    lax.fori_loop(0, pairs_ref.shape[1], enlist_targets, 0)

    def one_side(side, carry):
        q_at = pl.multiple_of(side * SIDE, 16)
        live = jnp.where(side == 0, naming, counts_ref[0])
        list_ref[side, live] = list_ref[side, 0]
        for c in range(helpers):
            scaled_ref[pl.ds(c * SHARD, SHARD), :] = query_refs[c][pl.ds(q_at, SHARD), :] * jnp.asarray(
                2.0 / (WIDTH * TEMPER), BF16
            )
        sum_ref[...] = jnp.zeros(sum_ref.shape, F32)
        acc_ref[...] = jnp.zeros(acc_ref.shape, F32)
        turns = (live + 1) // 2

        def biases(t):
            left = of_three(key_ref[list_ref[side, 2 * t], pl.ds(SHARD, 16), :])
            right = of_three(key_ref[list_ref[side, 2 * t + 1], pl.ds(SHARD, 16), :])
            return left, jnp.where(2 * t + 1 < live, right, LOW)

        def scores(t, shift, rows):
            first = key_ref[list_ref[side, 2 * t], pl.ds(0, SHARD), :]
            second = key_ref[list_ref[side, 2 * t + 1], pl.ds(0, SHARD), :]
            key = jnp.concatenate([first, second], axis=0)
            left, right = biases(t)
            cross = lax.dot_general(scaled_ref[rows, :], key, LANES, preferred_element_type=F32)
            return cross[:, :SHARD] + (left - shift), cross[:, SHARD:] + (right - shift), key

        def add(left, right, key, rows):
            left = jnp.exp(left)
            right = jnp.exp(right)
            sum_ref[rows, :] += left + right
            weight = jnp.concatenate([left.astype(BF16), right.astype(BF16)], axis=1)
            acc_ref[rows, :] += jnp.dot(weight, key, preferred_element_type=F32)

        @pl.when(safe)
        def _():
            def top_bias(t, top):
                left, right = biases(t)
                return jnp.maximum(top, jnp.maximum(left, right))

            top = lax.fori_loop(0, turns, top_bias, jnp.full((1, WIDTH), LOW, F32))
            top = jnp.max(top, axis=1, keepdims=True)
            shift_ref[...] = jnp.broadcast_to(top, shift_ref.shape)

            def add_up(t, carry):
                rows = pl.ds(0, helpers * SHARD)
                add(*scores(t, top, rows), rows)
                return carry

            lax.fori_loop(0, turns, add_up, 0)

        @pl.when(jnp.logical_not(safe))
        def _():
            def one_part(c, carry):
                rows = pl.ds(pl.multiple_of(c * SHARD, SHARD), SHARD)

                def find_peak(t, peak):
                    left, right, _ = scores(t, 0.0, rows)
                    return jnp.maximum(peak, jnp.maximum(left, right))

                peak = lax.fori_loop(0, turns, find_peak, jnp.full((SHARD, WIDTH), LOW, F32))
                top = jnp.broadcast_to(jnp.max(peak, axis=1, keepdims=True), (SHARD, WIDTH))
                shift_ref[:, rows] = top.T[:16]

                def add_up(t, carry):
                    left, right, key = scores(t, 0.0, rows)
                    add(left - top, right - top, key, rows)
                    return carry

                return lax.fori_loop(0, turns, add_up, carry)

            lax.fori_loop(0, helpers, one_part, 0)

        whole = sum_ref[...]
        hi = whole.astype(BF16)
        mid = (whole - hi.astype(F32)).astype(BF16)
        ones = jnp.ones((WIDTH, WIDTH), BF16)
        across = jnp.dot(hi, ones, preferred_element_type=F32) + jnp.dot(mid, ones, preferred_element_type=F32)
        mean = (acc_ref[...] * (1.0 / across)).astype(BF16)
        few = jnp.ones((16, WIDTH), BF16)
        total = lax.dot_general(few, hi, LANES, preferred_element_type=F32)
        total += lax.dot_general(few, mid, LANES, preferred_element_type=F32)
        lse = in_three(shift_ref[...] + jnp.log(total)).astype(BF16)
        for c in range(helpers):
            rows = slice(c * SHARD, (c + 1) * SHARD)
            out_ref, to = out_refs[c % CS], -(c // CS) % YS
            out_ref[to, pl.ds(q_at, SHARD), :] = mean[rows]
            out_ref[to, pl.ds(pl.multiple_of(q_at + SHARD, 16), 16), :] = lse[:, rows]
        return carry

    lax.fori_loop(0, 2, one_side, 0)


def merge_kernel(own_ref, other_ref, *refs):
    *out_refs, scr_ref = refs
    cases = [(k, side * SIDE) for k in range(len(out_refs)) for side in range(2)]
    scr_ref[...] = jnp.zeros(scr_ref.shape, F32)
    for n, (k, at) in enumerate(cases):
        own = of_three(own_ref[k, pl.ds(at + SHARD, 16), :])
        other = of_three(other_ref[k, pl.ds(at + SHARD, 16), :])
        top = jnp.maximum(own, other)
        share = jnp.exp(own - top)
        total = share + jnp.exp(other - top)
        scr_ref[pl.ds(n, 1), :] = share / total
        lse = jnp.broadcast_to(top + jnp.log(total), (16, SHARD))
        out_refs[k][pl.ds(at + SHARD, 16), :] = in_three(lse).astype(BF16)
    columns = scr_ref[...].T
    for n, (k, at) in enumerate(cases):
        own = own_ref[k, pl.ds(at, SHARD), :].astype(F32)
        other = other_ref[k, pl.ds(at, SHARD), :].astype(F32)
        out_refs[k][pl.ds(at, SHARD), :] = (other + columns[:, n : n + 1] * (own - other)).astype(BF16)


def settle_kernel(*refs):
    got_refs, refs = refs[:YS], refs[YS:]
    tp_ref, sp_ref, ntp_ref, level_ref, nsp_ref, *msg_refs, scr_ref = refs
    for side, old_ref, new_ref in ((0, tp_ref, ntp_ref), (1, sp_ref, nsp_ref)):
        at = side * SIDE
        parts = [of_three(ref[pl.ds(at + SHARD, 16), :]) for ref in got_refs]
        top = functools.reduce(jnp.maximum, parts)
        shares = [jnp.exp(part - top) for part in parts]
        total = functools.reduce(jnp.add, shares)
        scr_ref[...] = jnp.zeros(scr_ref.shape, F32)
        for h, share in enumerate(shares):
            scr_ref[pl.ds(h, 1), :] = share / total
        columns = scr_ref[...].T
        mean = jnp.zeros((SHARD, WIDTH), F32)
        for h, ref in enumerate(got_refs):
            mean = mean + columns[:, h : h + 1] * ref[pl.ds(at, SHARD), :].astype(F32)
        old = old_ref[pl.ds(0, SHARD), :]
        square = square_row(old.astype(BF16))
        level = -TEMPER * (top + jnp.log(total) - square * (1.0 / (WIDTH * TEMPER)))
        new = old + STRIDE * (mean - old)
        new_ref[pl.ds(0, SHARD), :] = new
        if side:
            new_ref[pl.ds(SHARD, 8), :] = level[:8]
        else:
            level_ref[...] = level[:1]
        if msg_refs:
            write_side(*msg_refs, side, new, level)


def finish_kernel(at_ref, *refs):
    own_ref, other_ref, points_ref, level_ref = refs
    for n in range(YS * CS):
        ref = (own_ref, other_ref)[n % CS].at[n // CS]
        helper = ((at_ref[2] - n // CS) & (YS - 1)) * CS + ((at_ref[3] + n) & (CS - 1))
        points_ref[0, pl.ds(pl.multiple_of(helper * SHARD, SHARD), SHARD), :] = ref[pl.ds(0, SHARD), :]
        level_ref[pl.ds(helper, 1), :] = ref[pl.ds(SHARD, 1), :]


def near_core(*arrays):
    return [pltpu.with_memory_space_constraint(x, pltpu.VMEM) for x in arrays]


def exchanged(copies, axes):
    return lax.all_to_all(copies, axes, split_axis=0, concat_axis=0, tiled=True)


def shifted(x, axis, step):
    n = lax.axis_size(axis)
    return lax.ppermute(x, axis, [(i, (i + step) % n) for i in range(n)])


def from_helpers(msg):
    pair = jnp.stack([msg, shifted(msg, "c", 1)])
    return [shifted(pair, "y", k) if k else pair for k in range(YS)]


def from_helpers_late(msg):
    own = jnp.stack([shifted(msg, "y", k) if k else msg for k in range(YS)])
    return own, shifted(own, "c", 1)


def from_blocks(copies, source):
    sides = [source] + [shifted(source, "x", k) for k in range(1, XS)]
    near = exchanged(copies, "z")
    ring = [None] * ZS
    ring[0] = ahead = back = jnp.stack(sides)
    targets = [near]
    for k in range(1, XS):
        targets.append(shifted(near, "x", k))
    for k in range(1, ZS // 2 + 1):
        ring[k] = ahead = shifted(ahead, "z", 1)
        if k < ZS // 2:
            ring[ZS - k] = back = shifted(back, "z", ZS - 1)
    return targets, ring


def on_device(
    source_points, source_potential, target_points, target_potential, pairs, counts, owner
):
    helper = lax.axis_index(HELP)
    block = lax.axis_index(("x", "z"))
    blocks = XS * ZS
    helpers = YS * CS
    at = jnp.stack([lax.axis_index(axis) for axis in ("x", "z", "y", "c")])
    smem = pl.BlockSpec(memory_space=pltpu.SMEM)
    vmem = pl.BlockSpec(memory_space=pltpu.VMEM)
    msg_shape = pltpu.VMEM((MSG, WIDTH), BF16)
    copies_shape = pltpu.VMEM((ZS, SIDE, WIDTH), BF16)
    source_shape = pltpu.VMEM((SIDE, WIDTH), BF16)
    half_shape = pltpu.VMEM((YS, MSG, WIDTH), BF16)
    final_shape = pltpu.VMEM((SHARD + 8, WIDTH), F32)
    own_points = pl.BlockSpec((1, SHARD, WIDTH), lambda i, at: (0, at[2] * CS + at[3], 0))
    own_level = pl.BlockSpec((1, SHARD), lambda i, at: (0, at[2] * CS + at[3]))
    whole = lambda *shape: pl.BlockSpec(shape, lambda i, at: (0,) * len(shape))
    msg, copies, source = pl.pallas_call(
        prepare_kernel,
        out_shape=(msg_shape, copies_shape, source_shape),
        grid_spec=pltpu.PrefetchScalarGridSpec(
            num_scalar_prefetch=1,
            grid=(1,),
            in_specs=[smem, smem, smem, whole(1, SHARD, WIDTH), whole(1, SHARD), own_points, own_level],
            out_specs=(whole(*msg_shape.shape), whole(*copies_shape.shape), whole(*source_shape.shape)),
        ),
        name="prepare",
    )(at, pairs, counts, owner, target_points, target_potential, source_points, source_potential)
    tp = target_points[0]
    sp = lax.dynamic_slice_in_dim(source_points[0], helper * SHARD, SHARD, 0)
    points_shape = jax.ShapeDtypeStruct((SHARD, WIDTH), F32)
    kept_shape = pltpu.VMEM((SHARD, WIDTH), F32)
    level_shape = jax.ShapeDtypeStruct((1, SHARD), F32)
    named = None
    for step in range(ITERS):
        targets, sources = from_blocks(copies, source)
        query = from_helpers(msg)
        if named is None:
            meta = jnp.concatenate([part[:, SHARD + META, :blocks] for part in targets])
            named = lax.dynamic_index_in_dim(meta, block, 1, False).astype(jnp.int32)
        own, other = pl.pallas_call(
            attend_kernel,
            out_shape=(half_shape, half_shape),
            in_specs=[smem] * 5 + [vmem] * (XS + ZS + YS),
            out_specs=(vmem, vmem),
            scratch_shapes=[
                pltpu.SMEM((2, blocks + 1), jnp.int32),
                pltpu.VMEM((2 * blocks, SIDE, WIDTH), BF16),
                pltpu.VMEM((helpers * SHARD, WIDTH), BF16),
                pltpu.VMEM((16, helpers * SHARD), F32),
                pltpu.VMEM((helpers * SHARD, WIDTH), F32),
                pltpu.VMEM((helpers * SHARD, WIDTH), F32),
            ],
            name="attend",
        )(
            at, pairs, counts, owner, named,
            targets[0], *near_core(*targets[1:]),
            *sources[: ZS // 2], *near_core(*sources[ZS // 2 : ZS // 2 + 2]), *sources[ZS // 2 + 2 :],
            query[0], *near_core(*query[1:]),
        )
        other = shifted(other, "c", 1)
        merged = pl.pallas_call(
            merge_kernel,
            out_shape=(msg_shape,) * YS,
            in_specs=[vmem, vmem],
            out_specs=(vmem,) * YS,
            scratch_shapes=[pltpu.VMEM((WIDTH, SHARD), F32)],
            name="merge",
        )(*near_core(own, other))
        got = [shifted(part, "y", k) if k else part for k, part in enumerate(merged)]
        last = step == ITERS - 1
        messages = () if last else (msg_shape, copies_shape, source_shape)
        tp, tl, sp, *rest = pl.pallas_call(
            settle_kernel,
            out_shape=(points_shape if last else kept_shape, level_shape, final_shape, *messages),
            in_specs=[vmem] * (YS + 2),
            out_specs=(vmem,) * (3 + len(messages)),
            scratch_shapes=[pltpu.VMEM((WIDTH, SHARD), F32)],
            name="settle",
        )(*near_core(*got), *((tp, sp) if step == 0 else near_core(tp, sp)))
        msg, copies, source = rest or (None,) * 3
    new_source_points, new_source_potential = pl.pallas_call(
        finish_kernel,
        out_shape=(jax.ShapeDtypeStruct(source_points.shape, F32), jax.ShapeDtypeStruct((helpers, SHARD), F32)),
        in_specs=[smem, vmem, vmem],
        out_specs=(vmem, vmem),
        name="finish",
    )(at, *near_core(*from_helpers_late(sp)))
    return new_source_points, new_source_potential.reshape(source_potential.shape), tp[None], tl


def solution(mesh):
    torus = Mesh(mesh.devices.reshape(XS, ZS, YS, CS), ("x", "z", "y", "c"))
    blk = ("x", "z")
    in_specs = (
        P(blk, None, None),
        P(blk, None),
        P(blk, HELP, None),
        P(blk, HELP),
        P(blk, None),
        P(blk),
        P(),
    )
    out_specs = (P(blk, None, None), P(blk, None), P(blk, HELP, None), P(blk, HELP))
    return jax.shard_map(
        on_device, mesh=torus, in_specs=in_specs, out_specs=out_specs, check_vma=False
    )
```

```python
import functools

import jax
import jax.numpy as jnp
from jax import lax
from jax.experimental import pallas as pl
from jax.experimental.pallas import tpu as pltpu
from jax.sharding import Mesh
from jax.sharding import PartitionSpec as P

ITERS = 2
HELP = ("y", "c")
SHARD = 128
WIDTH = 128
SIDE = SHARD + 16
MSG = 2 * SIDE
META = 8
SQUARE = 9
LIMIT = 40.0
XS, ZS, YS, CS = 4, 8, 4, 2
TEMPER = 0.25
STRIDE = 0.5
LOW = -1e30

F32 = jnp.float32
BF16 = jnp.bfloat16
LANES = (((1,), (1,)), ((), ()))


def as_row(column):
    return jnp.broadcast_to(column, (SHARD, WIDTH)).T[:16]


def in_three(rows):
    hi = rows.astype(BF16)
    rest = rows - hi.astype(F32)
    mid = rest.astype(BF16)
    lo = (rest - mid.astype(F32)).astype(BF16)
    at = lax.broadcasted_iota(jnp.int32, rows.shape, 0)
    out = jnp.where(at == 0, hi.astype(F32), jnp.where(at == 1, mid.astype(F32), lo.astype(F32)))
    return jnp.where(at < 3, out, 0.0)


def of_three(rows):
    rows = rows.astype(F32)
    return rows[0:1] + rows[1:2] + rows[2:3]


def square_row(rounded):
    wide = rounded.astype(F32)
    return as_row(jnp.sum(wide * wide, axis=1, keepdims=True))


def write_side(msg_ref, copies_ref, source_ref, side, points, level_row, meta=None):
    rounded = points.astype(BF16)
    square = square_row(rounded)
    bias = level_row * (1.0 / TEMPER) - square * (1.0 / (WIDTH * TEMPER))
    at = lax.broadcasted_iota(jnp.int32, square.shape, 0)
    extras = jnp.where(at == SQUARE, square, in_three(bias))
    if meta is not None:
        extras = jnp.where(at == META, meta, extras)
    extras = extras.astype(BF16)
    msg_ref[pl.ds(side * SIDE, SHARD), :] = rounded
    msg_ref[pl.ds(side * SIDE + SHARD, 16), :] = extras
    if side == 0:
        for k in range(copies_ref.shape[0]):
            copies_ref[k, pl.ds(0, SHARD), :] = rounded
            copies_ref[k, pl.ds(SHARD, 16), :] = extras
    else:
        source_ref[pl.ds(0, SHARD), :] = rounded
        source_ref[pl.ds(SHARD, 16), :] = extras


def prepare_kernel(
    at_ref, pairs_ref, counts_ref, owner_ref, tp_ref, tl_ref, sp_ref, sl_ref, msg_ref, copies_ref, source_ref
):
    lane = lax.broadcasted_iota(jnp.int32, (1, WIDTH), 1)
    meta = jnp.zeros((1, WIDTH), F32)
    count = counts_ref[0]
    for slot in range(pairs_ref.shape[1]):
        partner = jnp.where(slot < count, owner_ref[pairs_ref[0, slot]], -1)
        meta = jnp.where(lane == partner, 1.0, meta)
    write_side(msg_ref, copies_ref, source_ref, 0, tp_ref[0], tl_ref[...], meta)
    write_side(msg_ref, copies_ref, source_ref, 1, sp_ref[0], sl_ref[...])


def attend_kernel(at_ref, pairs_ref, counts_ref, owner_ref, named_ref, *refs):
    far, ring, helpers = XS, ZS, YS * CS
    target_refs, refs = refs[:far], refs[far:]
    source_refs, refs = refs[:ring], refs[ring:]
    query_refs, refs = [ref.at[n] for ref in refs[:2] for n in range(helpers // 2)], refs[2:]
    *out_refs, list_ref, key_ref, scaled_ref, shift_ref, sum_ref, acc_ref = refs
    at_x, at_z = at_ref[0], at_ref[1]
    blocks = far * ring
    for k in range(ring):
        key_ref[pl.ds(k * far, far)] = source_refs[k][...]
    for k in range(far):
        key_ref[pl.ds(blocks + k * ring, ring)] = target_refs[k][...]

    def largest(extras):
        top = functools.reduce(jnp.maximum, extras).astype(F32)
        return jnp.max(top[SQUARE : SQUARE + 1])

    bound = largest([key_ref[j, pl.ds(SHARD, 16), :] for j in range(2 * blocks)]) * largest(
        [ref[pl.ds(at, 16), :] for ref in query_refs for at in (SHARD, SIDE + SHARD)]
    )
    safe = bound * 1.03 <= (LIMIT * WIDTH * TEMPER / 2.0) ** 2

    def enlist_sources(j, count):
        list_ref[0, count] = ((at_z - j) & (ring - 1)) * far + j // ring
        return count + jnp.where(named_ref[j] > 0, 1, 0)

    def enlist_targets(s, carry):
        block = owner_ref[pairs_ref[0, s]]
        list_ref[1, s] = blocks + ((at_x - block // ring) & (far - 1)) * ring + (block & (ring - 1))
        return carry

    naming = lax.fori_loop(0, blocks, enlist_sources, 0)
    lax.fori_loop(0, pairs_ref.shape[1], enlist_targets, 0)

    def one_side(side, carry):
        q_at = pl.multiple_of(side * SIDE, 16)
        live = jnp.where(side == 0, naming, counts_ref[0])
        list_ref[side, live] = list_ref[side, 0]
        for c in range(helpers):
            scaled_ref[pl.ds(c * SHARD, SHARD), :] = query_refs[c][pl.ds(q_at, SHARD), :] * jnp.asarray(
                2.0 / (WIDTH * TEMPER), BF16
            )
        sum_ref[...] = jnp.zeros(sum_ref.shape, F32)
        acc_ref[...] = jnp.zeros(acc_ref.shape, F32)
        turns = (live + 1) // 2

        def biases(t):
            left = of_three(key_ref[list_ref[side, 2 * t], pl.ds(SHARD, 16), :])
            right = of_three(key_ref[list_ref[side, 2 * t + 1], pl.ds(SHARD, 16), :])
            return left, jnp.where(2 * t + 1 < live, right, LOW)

        def scores(t, shift, rows):
            first = key_ref[list_ref[side, 2 * t], pl.ds(0, SHARD), :]
            second = key_ref[list_ref[side, 2 * t + 1], pl.ds(0, SHARD), :]
            key = jnp.concatenate([first, second], axis=0)
            left, right = biases(t)
            cross = lax.dot_general(scaled_ref[rows, :], key, LANES, preferred_element_type=F32)
            return cross[:, :SHARD] + (left - shift), cross[:, SHARD:] + (right - shift), key

        def add(left, right, key, rows):
            left = jnp.exp(left)
            right = jnp.exp(right)
            sum_ref[rows, :] += left + right
            weight = jnp.concatenate([left.astype(BF16), right.astype(BF16)], axis=1)
            acc_ref[rows, :] += jnp.dot(weight, key, preferred_element_type=F32)

        @pl.when(safe)
        def _():
            def top_bias(t, top):
                left, right = biases(t)
                return jnp.maximum(top, jnp.maximum(left, right))

            top = lax.fori_loop(0, turns, top_bias, jnp.full((1, WIDTH), LOW, F32))
            top = jnp.max(top, axis=1, keepdims=True)
            shift_ref[...] = jnp.broadcast_to(top, shift_ref.shape)

            def add_up(t, carry):
                rows = pl.ds(0, helpers * SHARD)
                add(*scores(t, top, rows), rows)
                return carry

            lax.fori_loop(0, turns, add_up, 0)

        @pl.when(jnp.logical_not(safe))
        def _():
            def one_part(c, carry):
                rows = pl.ds(pl.multiple_of(c * SHARD, SHARD), SHARD)

                def find_peak(t, peak):
                    left, right, _ = scores(t, 0.0, rows)
                    return jnp.maximum(peak, jnp.maximum(left, right))

                peak = lax.fori_loop(0, turns, find_peak, jnp.full((SHARD, WIDTH), LOW, F32))
                top = jnp.broadcast_to(jnp.max(peak, axis=1, keepdims=True), (SHARD, WIDTH))
                shift_ref[:, rows] = top.T[:16]

                def add_up(t, carry):
                    left, right, key = scores(t, 0.0, rows)
                    add(left - top, right - top, key, rows)
                    return carry

                return lax.fori_loop(0, turns, add_up, carry)

            lax.fori_loop(0, helpers, one_part, 0)

        whole = sum_ref[...]
        hi = whole.astype(BF16)
        mid = (whole - hi.astype(F32)).astype(BF16)
        ones = jnp.ones((WIDTH, WIDTH), BF16)
        across = jnp.dot(hi, ones, preferred_element_type=F32) + jnp.dot(mid, ones, preferred_element_type=F32)
        mean = (acc_ref[...] * (1.0 / across)).astype(BF16)
        few = jnp.ones((16, WIDTH), BF16)
        total = lax.dot_general(few, hi, LANES, preferred_element_type=F32)
        total += lax.dot_general(few, mid, LANES, preferred_element_type=F32)
        lse = in_three(shift_ref[...] + jnp.log(total)).astype(BF16)
        for c in range(helpers):
            rows = slice(c * SHARD, (c + 1) * SHARD)
            out_ref, to = out_refs[c % CS], c // CS
            out_ref[to, pl.ds(q_at, SHARD), :] = mean[rows]
            out_ref[to, pl.ds(pl.multiple_of(q_at + SHARD, 16), 16), :] = lse[:, rows]
        return carry

    lax.fori_loop(0, 2, one_side, 0)


def merge_kernel(own_ref, other_ref, *refs):
    *out_refs, scr_ref = refs
    cases = [(k, side * SIDE) for k in range(len(out_refs)) for side in range(2)]
    scr_ref[...] = jnp.zeros(scr_ref.shape, F32)
    for n, (k, at) in enumerate(cases):
        own = of_three(own_ref[k, pl.ds(at + SHARD, 16), :])
        other = of_three(other_ref[k, pl.ds(at + SHARD, 16), :])
        top = jnp.maximum(own, other)
        share = jnp.exp(own - top)
        total = share + jnp.exp(other - top)
        scr_ref[pl.ds(n, 1), :] = share / total
        lse = jnp.broadcast_to(top + jnp.log(total), (16, SHARD))
        out_refs[k][pl.ds(at + SHARD, 16), :] = in_three(lse).astype(BF16)
    columns = scr_ref[...].T
    for n, (k, at) in enumerate(cases):
        own = own_ref[k, pl.ds(at, SHARD), :].astype(F32)
        other = other_ref[k, pl.ds(at, SHARD), :].astype(F32)
        out_refs[k][pl.ds(at, SHARD), :] = (other + columns[:, n : n + 1] * (own - other)).astype(BF16)


def settle_kernel(*refs):
    got_refs, refs = refs[:YS], refs[YS:]
    tp_ref, sp_ref, ntp_ref, level_ref, nsp_ref, *msg_refs, scr_ref = refs
    for side, old_ref, new_ref in ((0, tp_ref, ntp_ref), (1, sp_ref, nsp_ref)):
        at = side * SIDE
        parts = [of_three(ref[pl.ds(at + SHARD, 16), :]) for ref in got_refs]
        top = functools.reduce(jnp.maximum, parts)
        shares = [jnp.exp(part - top) for part in parts]
        total = functools.reduce(jnp.add, shares)
        scr_ref[...] = jnp.zeros(scr_ref.shape, F32)
        for h, share in enumerate(shares):
            scr_ref[pl.ds(h, 1), :] = share / total
        columns = scr_ref[...].T
        mean = jnp.zeros((SHARD, WIDTH), F32)
        for h, ref in enumerate(got_refs):
            mean = mean + columns[:, h : h + 1] * ref[pl.ds(at, SHARD), :].astype(F32)
        old = old_ref[pl.ds(0, SHARD), :]
        square = square_row(old.astype(BF16))
        level = -TEMPER * (top + jnp.log(total) - square * (1.0 / (WIDTH * TEMPER)))
        new = old + STRIDE * (mean - old)
        new_ref[pl.ds(0, SHARD), :] = new
        if side:
            new_ref[pl.ds(SHARD, 8), :] = level[:8]
        else:
            level_ref[...] = level[:1]
        if msg_refs:
            write_side(*msg_refs, side, new, level)


def finish_kernel(at_ref, *refs):
    own_ref, other_ref, points_ref, level_ref = refs
    for n in range(YS * CS):
        ref = (own_ref, other_ref)[n % CS].at[n // CS]
        helper = ((at_ref[2] - n // CS) & (YS - 1)) * CS + ((at_ref[3] + n) & (CS - 1))
        points_ref[0, pl.ds(pl.multiple_of(helper * SHARD, SHARD), SHARD), :] = ref[pl.ds(0, SHARD), :]
        level_ref[pl.ds(helper, 1), :] = ref[pl.ds(SHARD, 1), :]


def near_core(*arrays):
    return [pltpu.with_memory_space_constraint(x, pltpu.VMEM) for x in arrays]


def exchanged(copies, axes):
    return lax.all_to_all(copies, axes, split_axis=0, concat_axis=0, tiled=True)


def shifted(x, axis, step):
    n = lax.axis_size(axis)
    return lax.ppermute(x, axis, [(i, (i + step) % n) for i in range(n)])


def crossed(x, axis, bit):
    return lax.ppermute(x, axis, [(i, i ^ bit) for i in range(lax.axis_size(axis))])


def from_helpers(msg):
    near = jnp.stack([msg, crossed(msg, "c", 1)])
    near = jnp.concatenate([near, crossed(near, "y", 1)])
    return near, crossed(near, "y", 2)


def from_helpers_late(msg):
    own = jnp.stack([shifted(msg, "y", k) if k else msg for k in range(YS)])
    return own, shifted(own, "c", 1)


def from_blocks(copies, source):
    sides = [source] + [shifted(source, "x", k) for k in range(1, XS)]
    near = exchanged(copies, "z")
    ring = [None] * ZS
    ring[0] = ahead = back = jnp.stack(sides)
    targets = [near]
    for k in range(1, XS):
        targets.append(shifted(near, "x", k))
    for k in range(1, ZS // 2 + 1):
        ring[k] = ahead = shifted(ahead, "z", 1)
        if k < ZS // 2:
            ring[ZS - k] = back = shifted(back, "z", ZS - 1)
    return targets, ring


def on_device(
    source_points, source_potential, target_points, target_potential, pairs, counts, owner
):
    helper = lax.axis_index(HELP)
    block = lax.axis_index(("x", "z"))
    blocks = XS * ZS
    helpers = YS * CS
    at = jnp.stack([lax.axis_index(axis) for axis in ("x", "z", "y", "c")])
    smem = pl.BlockSpec(memory_space=pltpu.SMEM)
    vmem = pl.BlockSpec(memory_space=pltpu.VMEM)
    msg_shape = pltpu.VMEM((MSG, WIDTH), BF16)
    copies_shape = pltpu.VMEM((ZS, SIDE, WIDTH), BF16)
    source_shape = pltpu.VMEM((SIDE, WIDTH), BF16)
    half_shape = pltpu.VMEM((YS, MSG, WIDTH), BF16)
    final_shape = pltpu.VMEM((SHARD + 8, WIDTH), F32)
    own_points = pl.BlockSpec((1, SHARD, WIDTH), lambda i, at: (0, at[2] * CS + at[3], 0))
    own_level = pl.BlockSpec((1, SHARD), lambda i, at: (0, at[2] * CS + at[3]))
    whole = lambda *shape: pl.BlockSpec(shape, lambda i, at: (0,) * len(shape))
    msg, copies, source = pl.pallas_call(
        prepare_kernel,
        out_shape=(msg_shape, copies_shape, source_shape),
        grid_spec=pltpu.PrefetchScalarGridSpec(
            num_scalar_prefetch=1,
            grid=(1,),
            in_specs=[smem, smem, smem, whole(1, SHARD, WIDTH), whole(1, SHARD), own_points, own_level],
            out_specs=(whole(*msg_shape.shape), whole(*copies_shape.shape), whole(*source_shape.shape)),
        ),
        name="prepare",
    )(at, pairs, counts, owner, target_points, target_potential, source_points, source_potential)
    tp = target_points[0]
    sp = lax.dynamic_slice_in_dim(source_points[0], helper * SHARD, SHARD, 0)
    points_shape = jax.ShapeDtypeStruct((SHARD, WIDTH), F32)
    kept_shape = pltpu.VMEM((SHARD, WIDTH), F32)
    level_shape = jax.ShapeDtypeStruct((1, SHARD), F32)
    named = None
    for step in range(ITERS):
        targets, sources = from_blocks(copies, source)
        query = from_helpers(msg)
        if named is None:
            meta = jnp.concatenate([part[:, SHARD + META, :blocks] for part in targets])
            named = lax.dynamic_index_in_dim(meta, block, 1, False).astype(jnp.int32)
        own, other = pl.pallas_call(
            attend_kernel,
            out_shape=(half_shape, half_shape),
            in_specs=[smem] * 5 + [vmem] * (XS + ZS + 2),
            out_specs=(vmem, vmem),
            scratch_shapes=[
                pltpu.SMEM((2, blocks + 1), jnp.int32),
                pltpu.VMEM((2 * blocks, SIDE, WIDTH), BF16),
                pltpu.VMEM((helpers * SHARD, WIDTH), BF16),
                pltpu.VMEM((16, helpers * SHARD), F32),
                pltpu.VMEM((helpers * SHARD, WIDTH), F32),
                pltpu.VMEM((helpers * SHARD, WIDTH), F32),
            ],
            name="attend",
        )(
            at, pairs, counts, owner, named,
            targets[0], *near_core(*targets[1:]),
            *sources[: ZS // 2], *near_core(*sources[ZS // 2 : ZS // 2 + 2]), *sources[ZS // 2 + 2 :],
            query[0], *near_core(*query[1:]),
        )
        other = shifted(other, "c", 1)
        merged = pl.pallas_call(
            merge_kernel,
            out_shape=(msg_shape,) * YS,
            in_specs=[vmem, vmem],
            out_specs=(vmem,) * YS,
            scratch_shapes=[pltpu.VMEM((WIDTH, SHARD), F32)],
            name="merge",
        )(*near_core(own, other))
        got = [crossed(part, "y", k) if k else part for k, part in enumerate(merged)]
        last = step == ITERS - 1
        messages = () if last else (msg_shape, copies_shape, source_shape)
        tp, tl, sp, *rest = pl.pallas_call(
            settle_kernel,
            out_shape=(points_shape if last else kept_shape, level_shape, final_shape, *messages),
            in_specs=[vmem] * (YS + 2),
            out_specs=(vmem,) * (3 + len(messages)),
            scratch_shapes=[pltpu.VMEM((WIDTH, SHARD), F32)],
            name="settle",
        )(*near_core(*got), *((tp, sp) if step == 0 else near_core(tp, sp)))
        msg, copies, source = rest or (None,) * 3
    new_source_points, new_source_potential = pl.pallas_call(
        finish_kernel,
        out_shape=(jax.ShapeDtypeStruct(source_points.shape, F32), jax.ShapeDtypeStruct((helpers, SHARD), F32)),
        in_specs=[smem, vmem, vmem],
        out_specs=(vmem, vmem),
        name="finish",
    )(at, *near_core(*from_helpers_late(sp)))
    return new_source_points, new_source_potential.reshape(source_potential.shape), tp[None], tl


def solution(mesh):
    torus = Mesh(mesh.devices.reshape(XS, ZS, YS, CS), ("x", "z", "y", "c"))
    blk = ("x", "z")
    in_specs = (
        P(blk, None, None),
        P(blk, None),
        P(blk, HELP, None),
        P(blk, HELP),
        P(blk, None),
        P(blk),
        P(),
    )
    out_specs = (P(blk, None, None), P(blk, None), P(blk, HELP, None), P(blk, HELP))
    return jax.shard_map(
        on_device, mesh=torus, in_specs=in_specs, out_specs=out_specs, check_vma=False
    )
```

```python
import functools

import jax
import jax.numpy as jnp
from jax import lax
from jax.experimental import pallas as pl
from jax.experimental.pallas import tpu as pltpu
from jax.sharding import Mesh
from jax.sharding import PartitionSpec as P

ITERS = 2
HELP = ("y", "c")
SHARD = 128
WIDTH = 128
SIDE = SHARD + 16
MSG = 2 * SIDE
META = 8
SQUARE = 9
GROUP = 4
LIMIT = 40.0
XS, ZS, YS, CS = 4, 8, 4, 2
TEMPER = 0.25
STRIDE = 0.5
LOW = -1e30

F32 = jnp.float32
BF16 = jnp.bfloat16
LANES = (((1,), (1,)), ((), ()))


def as_row(column):
    return jnp.broadcast_to(column, (SHARD, WIDTH)).T[:16]


def in_three(rows):
    hi = rows.astype(BF16)
    rest = rows - hi.astype(F32)
    mid = rest.astype(BF16)
    lo = (rest - mid.astype(F32)).astype(BF16)
    at = lax.broadcasted_iota(jnp.int32, rows.shape, 0)
    out = jnp.where(at == 0, hi.astype(F32), jnp.where(at == 1, mid.astype(F32), lo.astype(F32)))
    return jnp.where(at < 3, out, 0.0)


def of_three(rows):
    rows = rows.astype(F32)
    return rows[0:1] + rows[1:2] + rows[2:3]


def square_row(rounded):
    wide = rounded.astype(F32)
    return as_row(jnp.sum(wide * wide, axis=1, keepdims=True))


def write_side(msg_ref, copies_ref, source_ref, side, points, level_row, meta=None):
    rounded = points.astype(BF16)
    square = square_row(rounded)
    bias = level_row * (1.0 / TEMPER) - square * (1.0 / (WIDTH * TEMPER))
    at = lax.broadcasted_iota(jnp.int32, square.shape, 0)
    extras = jnp.where(at == SQUARE, square, in_three(bias))
    if meta is not None:
        extras = jnp.where(at == META, meta, extras)
    extras = extras.astype(BF16)
    msg_ref[pl.ds(side * SIDE, SHARD), :] = rounded
    msg_ref[pl.ds(side * SIDE + SHARD, 16), :] = extras
    if side == 0:
        for k in range(copies_ref.shape[0]):
            copies_ref[k, pl.ds(0, SHARD), :] = rounded
            copies_ref[k, pl.ds(SHARD, 16), :] = extras
    else:
        source_ref[pl.ds(0, SHARD), :] = rounded
        source_ref[pl.ds(SHARD, 16), :] = extras


def prepare_kernel(
    at_ref, pairs_ref, counts_ref, owner_ref, tp_ref, tl_ref, sp_ref, sl_ref, msg_ref, copies_ref, source_ref
):
    lane = lax.broadcasted_iota(jnp.int32, (1, WIDTH), 1)
    meta = jnp.zeros((1, WIDTH), F32)
    count = counts_ref[0]
    for slot in range(pairs_ref.shape[1]):
        partner = jnp.where(slot < count, owner_ref[pairs_ref[0, slot]], -1)
        meta = jnp.where(lane == partner, 1.0, meta)
    write_side(msg_ref, copies_ref, source_ref, 0, tp_ref[0], tl_ref[...], meta)
    write_side(msg_ref, copies_ref, source_ref, 1, sp_ref[0], sl_ref[...])


def attend_kernel(at_ref, pairs_ref, counts_ref, owner_ref, named_ref, *refs):
    far, ring, helpers = XS, ZS, YS * CS
    target_refs, refs = refs[:far], refs[far:]
    source_refs, refs = refs[:ring], refs[ring:]
    query_refs, refs = [ref.at[n] for ref in refs[:2] for n in range(helpers // 2)], refs[2:]
    *out_refs, list_ref, key_ref, scaled_ref, shift_ref, sum_ref, acc_ref = refs
    at_x, at_z = at_ref[0], at_ref[1]
    blocks = far * ring
    for k in range(ring):
        key_ref[pl.ds(k * far, far)] = source_refs[k][...]
    for k in range(far):
        key_ref[pl.ds(blocks + k * ring, ring)] = target_refs[k][...]

    def largest(extras):
        top = functools.reduce(jnp.maximum, extras).astype(F32)
        return jnp.max(top[SQUARE : SQUARE + 1])

    bound = largest([key_ref[j, pl.ds(SHARD, 16), :] for j in range(2 * blocks)]) * largest(
        [ref[pl.ds(at, 16), :] for ref in query_refs for at in (SHARD, SIDE + SHARD)]
    )
    safe = bound * 1.03 <= (LIMIT * WIDTH * TEMPER / 2.0) ** 2

    def enlist_sources(j, count):
        list_ref[0, count] = ((at_z - j) & (ring - 1)) * far + j // ring
        return count + jnp.where(named_ref[j] > 0, 1, 0)

    def enlist_targets(s, carry):
        block = owner_ref[pairs_ref[0, s]]
        list_ref[1, s] = blocks + ((at_x - block // ring) & (far - 1)) * ring + (block & (ring - 1))
        return carry

    naming = lax.fori_loop(0, blocks, enlist_sources, 0)
    lax.fori_loop(0, pairs_ref.shape[1], enlist_targets, 0)

    def one_side(side, carry):
        q_at = pl.multiple_of(side * SIDE, 16)
        live = jnp.where(side == 0, naming, counts_ref[0])
        for n in range(GROUP - 1):
            list_ref[side, live + n] = list_ref[side, 0]
        for c in range(helpers):
            scaled_ref[pl.ds(c * SHARD, SHARD), :] = query_refs[c][pl.ds(q_at, SHARD), :] * jnp.asarray(
                2.0 / (WIDTH * TEMPER), BF16
            )
        sum_ref[...] = jnp.zeros(sum_ref.shape, F32)
        acc_ref[...] = jnp.zeros(acc_ref.shape, F32)
        turns = (live + GROUP - 1) // GROUP

        def biases(t):
            rows = [of_three(key_ref[list_ref[side, GROUP * t + n], pl.ds(SHARD, 16), :]) for n in range(GROUP)]
            return [jnp.where(GROUP * t + n < live, row, LOW) for n, row in enumerate(rows)]

        def scores(t, shift, rows):
            key = jnp.concatenate([key_ref[list_ref[side, GROUP * t + n], pl.ds(0, SHARD), :] for n in range(GROUP)])
            cross = lax.dot_general(scaled_ref[rows, :], key, LANES, preferred_element_type=F32)
            parts = [cross[:, n * SHARD : (n + 1) * SHARD] + (row - shift) for n, row in enumerate(biases(t))]
            return parts, key

        def add(parts, key, rows):
            parts = [jnp.exp(part) for part in parts]
            sum_ref[rows, :] += functools.reduce(jnp.add, parts)
            weight = jnp.concatenate([part.astype(BF16) for part in parts], axis=1)
            acc_ref[rows, :] += jnp.dot(weight, key, preferred_element_type=F32)

        @pl.when(safe)
        def _():
            def top_bias(t, top):
                return functools.reduce(jnp.maximum, biases(t), top)

            top = lax.fori_loop(0, turns, top_bias, jnp.full((1, WIDTH), LOW, F32))
            top = jnp.max(top, axis=1, keepdims=True)
            shift_ref[...] = jnp.broadcast_to(top, shift_ref.shape)

            def add_up(t, carry):
                rows = pl.ds(0, helpers * SHARD)
                add(*scores(t, top, rows), rows)
                return carry

            lax.fori_loop(0, turns, add_up, 0)

        @pl.when(jnp.logical_not(safe))
        def _():
            def one_part(c, carry):
                rows = pl.ds(pl.multiple_of(c * SHARD, SHARD), SHARD)

                def find_peak(t, peak):
                    return functools.reduce(jnp.maximum, scores(t, 0.0, rows)[0], peak)

                peak = lax.fori_loop(0, turns, find_peak, jnp.full((SHARD, WIDTH), LOW, F32))
                top = jnp.broadcast_to(jnp.max(peak, axis=1, keepdims=True), (SHARD, WIDTH))
                shift_ref[:, rows] = top.T[:16]

                def add_up(t, carry):
                    parts, key = scores(t, 0.0, rows)
                    add([part - top for part in parts], key, rows)
                    return carry

                return lax.fori_loop(0, turns, add_up, carry)

            lax.fori_loop(0, helpers, one_part, 0)

        whole = sum_ref[...]
        hi = whole.astype(BF16)
        mid = (whole - hi.astype(F32)).astype(BF16)
        ones = jnp.ones((WIDTH, WIDTH), BF16)
        across = jnp.dot(hi, ones, preferred_element_type=F32) + jnp.dot(mid, ones, preferred_element_type=F32)
        mean = (acc_ref[...] * (1.0 / across)).astype(BF16)
        few = jnp.ones((16, WIDTH), BF16)
        total = lax.dot_general(few, hi, LANES, preferred_element_type=F32)
        total += lax.dot_general(few, mid, LANES, preferred_element_type=F32)
        lse = in_three(shift_ref[...] + jnp.log(total)).astype(BF16)
        for c in range(helpers):
            rows = slice(c * SHARD, (c + 1) * SHARD)
            out_ref, to = out_refs[c % CS], c // CS
            out_ref[to, pl.ds(q_at, SHARD), :] = mean[rows]
            out_ref[to, pl.ds(pl.multiple_of(q_at + SHARD, 16), 16), :] = lse[:, rows]
        return carry

    lax.fori_loop(0, 2, one_side, 0)


def merge_kernel(own_ref, other_ref, *refs):
    *out_refs, scr_ref = refs
    cases = [(k, side * SIDE) for k in range(len(out_refs)) for side in range(2)]
    scr_ref[...] = jnp.zeros(scr_ref.shape, F32)
    for n, (k, at) in enumerate(cases):
        own = of_three(own_ref[k, pl.ds(at + SHARD, 16), :])
        other = of_three(other_ref[k, pl.ds(at + SHARD, 16), :])
        top = jnp.maximum(own, other)
        share = jnp.exp(own - top)
        total = share + jnp.exp(other - top)
        scr_ref[pl.ds(n, 1), :] = share / total
        lse = jnp.broadcast_to(top + jnp.log(total), (16, SHARD))
        out_refs[k][pl.ds(at + SHARD, 16), :] = in_three(lse).astype(BF16)
    columns = scr_ref[...].T
    for n, (k, at) in enumerate(cases):
        own = own_ref[k, pl.ds(at, SHARD), :].astype(F32)
        other = other_ref[k, pl.ds(at, SHARD), :].astype(F32)
        out_refs[k][pl.ds(at, SHARD), :] = (other + columns[:, n : n + 1] * (own - other)).astype(BF16)


def settle_kernel(*refs):
    got_refs, refs = refs[:YS], refs[YS:]
    tp_ref, sp_ref, ntp_ref, level_ref, nsp_ref, *msg_refs, scr_ref = refs
    for side, old_ref, new_ref in ((0, tp_ref, ntp_ref), (1, sp_ref, nsp_ref)):
        at = side * SIDE
        parts = [of_three(ref[pl.ds(at + SHARD, 16), :]) for ref in got_refs]
        top = functools.reduce(jnp.maximum, parts)
        shares = [jnp.exp(part - top) for part in parts]
        total = functools.reduce(jnp.add, shares)
        scr_ref[...] = jnp.zeros(scr_ref.shape, F32)
        for h, share in enumerate(shares):
            scr_ref[pl.ds(h, 1), :] = share / total
        columns = scr_ref[...].T
        mean = jnp.zeros((SHARD, WIDTH), F32)
        for h, ref in enumerate(got_refs):
            mean = mean + columns[:, h : h + 1] * ref[pl.ds(at, SHARD), :].astype(F32)
        old = old_ref[pl.ds(0, SHARD), :]
        square = square_row(old.astype(BF16))
        level = -TEMPER * (top + jnp.log(total) - square * (1.0 / (WIDTH * TEMPER)))
        new = old + STRIDE * (mean - old)
        new_ref[pl.ds(0, SHARD), :] = new
        if side:
            new_ref[pl.ds(SHARD, 8), :] = level[:8]
        else:
            level_ref[...] = level[:1]
        if msg_refs:
            write_side(*msg_refs, side, new, level)


def finish_kernel(at_ref, *refs):
    own_ref, other_ref, points_ref, level_ref = refs
    for n in range(YS * CS):
        ref = (own_ref, other_ref)[n % CS].at[n // CS]
        helper = ((at_ref[2] - n // CS) & (YS - 1)) * CS + ((at_ref[3] + n) & (CS - 1))
        points_ref[0, pl.ds(pl.multiple_of(helper * SHARD, SHARD), SHARD), :] = ref[pl.ds(0, SHARD), :]
        level_ref[pl.ds(helper, 1), :] = ref[pl.ds(SHARD, 1), :]


def near_core(*arrays):
    return [pltpu.with_memory_space_constraint(x, pltpu.VMEM) for x in arrays]


def exchanged(copies, axes):
    return lax.all_to_all(copies, axes, split_axis=0, concat_axis=0, tiled=True)


def shifted(x, axis, step):
    n = lax.axis_size(axis)
    return lax.ppermute(x, axis, [(i, (i + step) % n) for i in range(n)])


def crossed(x, axis, bit):
    return lax.ppermute(x, axis, [(i, i ^ bit) for i in range(lax.axis_size(axis))])


def from_helpers(msg):
    near = jnp.stack([msg, crossed(msg, "c", 1)])
    near = jnp.concatenate([near, crossed(near, "y", 1)])
    return near, crossed(near, "y", 2)


def from_helpers_late(msg):
    own = jnp.stack([shifted(msg, "y", k) if k else msg for k in range(YS)])
    return own, shifted(own, "c", 1)


def from_blocks(copies, source):
    sides = [source] + [shifted(source, "x", k) for k in range(1, XS)]
    near = exchanged(copies, "z")
    ring = [None] * ZS
    ring[0] = ahead = back = jnp.stack(sides)
    targets = [near]
    for k in range(1, XS):
        targets.append(shifted(near, "x", k))
    for k in range(1, ZS // 2 + 1):
        ring[k] = ahead = shifted(ahead, "z", 1)
        if k < ZS // 2:
            ring[ZS - k] = back = shifted(back, "z", ZS - 1)
    return targets, ring


def on_device(
    source_points, source_potential, target_points, target_potential, pairs, counts, owner
):
    helper = lax.axis_index(HELP)
    block = lax.axis_index(("x", "z"))
    blocks = XS * ZS
    helpers = YS * CS
    at = jnp.stack([lax.axis_index(axis) for axis in ("x", "z", "y", "c")])
    smem = pl.BlockSpec(memory_space=pltpu.SMEM)
    vmem = pl.BlockSpec(memory_space=pltpu.VMEM)
    msg_shape = pltpu.VMEM((MSG, WIDTH), BF16)
    copies_shape = pltpu.VMEM((ZS, SIDE, WIDTH), BF16)
    source_shape = pltpu.VMEM((SIDE, WIDTH), BF16)
    half_shape = pltpu.VMEM((YS, MSG, WIDTH), BF16)
    final_shape = pltpu.VMEM((SHARD + 8, WIDTH), F32)
    own_points = pl.BlockSpec((1, SHARD, WIDTH), lambda i, at: (0, at[2] * CS + at[3], 0))
    own_level = pl.BlockSpec((1, SHARD), lambda i, at: (0, at[2] * CS + at[3]))
    whole = lambda *shape: pl.BlockSpec(shape, lambda i, at: (0,) * len(shape))
    msg, copies, source = pl.pallas_call(
        prepare_kernel,
        out_shape=(msg_shape, copies_shape, source_shape),
        grid_spec=pltpu.PrefetchScalarGridSpec(
            num_scalar_prefetch=1,
            grid=(1,),
            in_specs=[smem, smem, smem, whole(1, SHARD, WIDTH), whole(1, SHARD), own_points, own_level],
            out_specs=(whole(*msg_shape.shape), whole(*copies_shape.shape), whole(*source_shape.shape)),
        ),
        name="prepare",
    )(at, pairs, counts, owner, target_points, target_potential, source_points, source_potential)
    tp = target_points[0]
    sp = lax.dynamic_slice_in_dim(source_points[0], helper * SHARD, SHARD, 0)
    points_shape = jax.ShapeDtypeStruct((SHARD, WIDTH), F32)
    kept_shape = pltpu.VMEM((SHARD, WIDTH), F32)
    level_shape = jax.ShapeDtypeStruct((1, SHARD), F32)
    named = None
    for step in range(ITERS):
        targets, sources = from_blocks(copies, source)
        query = from_helpers(msg)
        if named is None:
            meta = jnp.concatenate([part[:, SHARD + META, :blocks] for part in targets])
            named = lax.dynamic_index_in_dim(meta, block, 1, False).astype(jnp.int32)
        own, other = pl.pallas_call(
            attend_kernel,
            out_shape=(half_shape, half_shape),
            in_specs=[smem] * 5 + [vmem] * (XS + ZS + 2),
            out_specs=(vmem, vmem),
            scratch_shapes=[
                pltpu.SMEM((2, blocks + GROUP), jnp.int32),
                pltpu.VMEM((2 * blocks, SIDE, WIDTH), BF16),
                pltpu.VMEM((helpers * SHARD, WIDTH), BF16),
                pltpu.VMEM((16, helpers * SHARD), F32),
                pltpu.VMEM((helpers * SHARD, WIDTH), F32),
                pltpu.VMEM((helpers * SHARD, WIDTH), F32),
            ],
            name="attend",
        )(
            at, pairs, counts, owner, named,
            targets[0], *near_core(*targets[1:]),
            *sources[: ZS // 2], *near_core(*sources[ZS // 2 : ZS // 2 + 2]), *sources[ZS // 2 + 2 :],
            query[0], *near_core(*query[1:]),
        )
        other = shifted(other, "c", 1)
        merged = pl.pallas_call(
            merge_kernel,
            out_shape=(msg_shape,) * YS,
            in_specs=[vmem, vmem],
            out_specs=(vmem,) * YS,
            scratch_shapes=[pltpu.VMEM((WIDTH, SHARD), F32)],
            name="merge",
        )(*near_core(own, other))
        got = [crossed(part, "y", k) if k else part for k, part in enumerate(merged)]
        last = step == ITERS - 1
        messages = () if last else (msg_shape, copies_shape, source_shape)
        tp, tl, sp, *rest = pl.pallas_call(
            settle_kernel,
            out_shape=(points_shape if last else kept_shape, level_shape, final_shape, *messages),
            in_specs=[vmem] * (YS + 2),
            out_specs=(vmem,) * (3 + len(messages)),
            scratch_shapes=[pltpu.VMEM((WIDTH, SHARD), F32)],
            name="settle",
        )(*near_core(*got), *((tp, sp) if step == 0 else near_core(tp, sp)))
        msg, copies, source = rest or (None,) * 3
    new_source_points, new_source_potential = pl.pallas_call(
        finish_kernel,
        out_shape=(jax.ShapeDtypeStruct(source_points.shape, F32), jax.ShapeDtypeStruct((helpers, SHARD), F32)),
        in_specs=[smem, vmem, vmem],
        out_specs=(vmem, vmem),
        name="finish",
    )(at, *near_core(*from_helpers_late(sp)))
    return new_source_points, new_source_potential.reshape(source_potential.shape), tp[None], tl


def solution(mesh):
    torus = Mesh(mesh.devices.reshape(XS, ZS, YS, CS), ("x", "z", "y", "c"))
    blk = ("x", "z")
    in_specs = (
        P(blk, None, None),
        P(blk, None),
        P(blk, HELP, None),
        P(blk, HELP),
        P(blk, None),
        P(blk),
        P(),
    )
    out_specs = (P(blk, None, None), P(blk, None), P(blk, HELP, None), P(blk, HELP))
    return jax.shard_map(
        on_device, mesh=torus, in_specs=in_specs, out_specs=out_specs, check_vma=False
    )
```

```python
import functools

import jax
import jax.numpy as jnp
from jax import lax
from jax.experimental import pallas as pl
from jax.experimental.pallas import tpu as pltpu
from jax.sharding import Mesh
from jax.sharding import PartitionSpec as P

ITERS = 2
HELP = ("y", "c")
SHARD = 128
WIDTH = 128
SIDE = SHARD + 16
MSG = 2 * SIDE
META = 8
SQUARE = 9
GROUP = 4
LIMIT = 40.0
XS, ZS, YS, CS = 4, 8, 4, 2
TEMPER = 0.25
STRIDE = 0.5
LOW = -1e30

F32 = jnp.float32
BF16 = jnp.bfloat16
LANES = (((1,), (1,)), ((), ()))


def in_three(rows):
    hi = rows.astype(BF16)
    rest = rows - hi.astype(F32)
    mid = rest.astype(BF16)
    lo = (rest - mid.astype(F32)).astype(BF16)
    at = lax.broadcasted_iota(jnp.int32, rows.shape, 0)
    out = jnp.where(at == 0, hi.astype(F32), jnp.where(at == 1, mid.astype(F32), lo.astype(F32)))
    return jnp.where(at < 3, out, 0.0)


def of_three(rows):
    rows = rows.astype(F32)
    return rows[0:1] + rows[1:2] + rows[2:3]


def square_row(rounded):
    wide = rounded.astype(F32)
    square = wide * wide
    hi = square.astype(BF16)
    mid = (square - hi.astype(F32)).astype(BF16)
    ones = jnp.ones((16, WIDTH), BF16)
    return lax.dot_general(ones, hi, LANES, preferred_element_type=F32) + lax.dot_general(
        ones, mid, LANES, preferred_element_type=F32
    )


def write_side(msg_ref, copies_ref, source_ref, side, points, level_row, meta=None):
    rounded = points.astype(BF16)
    square = square_row(rounded)
    bias = level_row * (1.0 / TEMPER) - square * (1.0 / (WIDTH * TEMPER))
    at = lax.broadcasted_iota(jnp.int32, square.shape, 0)
    extras = jnp.where(at == SQUARE, square, in_three(bias))
    if meta is not None:
        extras = jnp.where(at == META, meta, extras)
    extras = extras.astype(BF16)
    msg_ref[pl.ds(side * SIDE, SHARD), :] = rounded
    msg_ref[pl.ds(side * SIDE + SHARD, 16), :] = extras
    if side == 0:
        for k in range(copies_ref.shape[0]):
            copies_ref[k, pl.ds(0, SHARD), :] = rounded
            copies_ref[k, pl.ds(SHARD, 16), :] = extras
    else:
        source_ref[pl.ds(0, SHARD), :] = rounded
        source_ref[pl.ds(SHARD, 16), :] = extras


def prepare_kernel(
    at_ref, pairs_ref, counts_ref, owner_ref, tp_ref, tl_ref, sp_ref, sl_ref, msg_ref, copies_ref, source_ref
):
    lane = lax.broadcasted_iota(jnp.int32, (1, WIDTH), 1)
    meta = jnp.zeros((1, WIDTH), F32)
    count = counts_ref[0]
    for slot in range(pairs_ref.shape[1]):
        partner = jnp.where(slot < count, owner_ref[pairs_ref[0, slot]], -1)
        meta = jnp.where(lane == partner, 1.0, meta)
    write_side(msg_ref, copies_ref, source_ref, 0, tp_ref[0], tl_ref[...], meta)
    write_side(msg_ref, copies_ref, source_ref, 1, sp_ref[0], sl_ref[...])


def attend_kernel(at_ref, pairs_ref, counts_ref, owner_ref, named_ref, *refs):
    far, ring, helpers = XS, ZS, YS * CS
    target_refs, refs = refs[:far], refs[far:]
    source_refs, refs = refs[:ring], refs[ring:]
    query_refs, refs = [ref.at[n] for ref in refs[:2] for n in range(helpers // 2)], refs[2:]
    *out_refs, list_ref, key_ref, scaled_ref, shift_ref, sum_ref, acc_ref = refs
    at_x, at_z = at_ref[0], at_ref[1]
    blocks = far * ring
    for k in range(ring):
        key_ref[pl.ds(k * far, far)] = source_refs[k][...]
    for k in range(far):
        key_ref[pl.ds(blocks + k * ring, ring)] = target_refs[k][...]

    def largest(extras):
        top = functools.reduce(jnp.maximum, extras).astype(F32)
        return jnp.max(top[SQUARE : SQUARE + 1])

    bound = largest([key_ref[j, pl.ds(SHARD, 16), :] for j in range(2 * blocks)]) * largest(
        [ref[pl.ds(at, 16), :] for ref in query_refs for at in (SHARD, SIDE + SHARD)]
    )
    safe = bound * 1.03 <= (LIMIT * WIDTH * TEMPER / 2.0) ** 2

    def enlist_sources(j, count):
        list_ref[0, count] = ((at_z - j) & (ring - 1)) * far + j // ring
        return count + jnp.where(named_ref[j] > 0, 1, 0)

    def enlist_targets(s, carry):
        block = owner_ref[pairs_ref[0, s]]
        list_ref[1, s] = blocks + ((at_x - block // ring) & (far - 1)) * ring + (block & (ring - 1))
        return carry

    naming = lax.fori_loop(0, blocks, enlist_sources, 0)
    lax.fori_loop(0, pairs_ref.shape[1], enlist_targets, 0)

    def one_side(side, carry):
        q_at = pl.multiple_of(side * SIDE, 16)
        live = jnp.where(side == 0, naming, counts_ref[0])
        for n in range(GROUP - 1):
            list_ref[side, live + n] = list_ref[side, 0]
        for c in range(helpers):
            scaled_ref[pl.ds(c * SHARD, SHARD), :] = query_refs[c][pl.ds(q_at, SHARD), :] * jnp.asarray(
                2.0 / (WIDTH * TEMPER), BF16
            )
        sum_ref[...] = jnp.zeros(sum_ref.shape, F32)
        acc_ref[...] = jnp.zeros(acc_ref.shape, F32)
        turns = (live + GROUP - 1) // GROUP

        def biases(t):
            rows = [of_three(key_ref[list_ref[side, GROUP * t + n], pl.ds(SHARD, 16), :]) for n in range(GROUP)]
            return [jnp.where(GROUP * t + n < live, row, LOW) for n, row in enumerate(rows)]

        def scores(t, shift, rows):
            key = jnp.concatenate([key_ref[list_ref[side, GROUP * t + n], pl.ds(0, SHARD), :] for n in range(GROUP)])
            cross = lax.dot_general(scaled_ref[rows, :], key, LANES, preferred_element_type=F32)
            parts = [cross[:, n * SHARD : (n + 1) * SHARD] + (row - shift) for n, row in enumerate(biases(t))]
            return parts, key

        def add(parts, key, rows):
            parts = [jnp.exp(part) for part in parts]
            sum_ref[rows, :] += functools.reduce(jnp.add, parts)
            weight = jnp.concatenate([part.astype(BF16) for part in parts], axis=1)
            acc_ref[rows, :] += jnp.dot(weight, key, preferred_element_type=F32)

        @pl.when(safe)
        def _():
            def top_bias(t, top):
                return functools.reduce(jnp.maximum, biases(t), top)

            top = lax.fori_loop(0, turns, top_bias, jnp.full((1, WIDTH), LOW, F32))
            top = jnp.max(top, axis=1, keepdims=True)
            shift_ref[...] = jnp.broadcast_to(top, shift_ref.shape)

            def add_up(t, carry):
                rows = pl.ds(0, helpers * SHARD)
                add(*scores(t, top, rows), rows)
                return carry

            lax.fori_loop(0, turns, add_up, 0)

        @pl.when(jnp.logical_not(safe))
        def _():
            def one_part(c, carry):
                rows = pl.ds(pl.multiple_of(c * SHARD, SHARD), SHARD)

                def find_peak(t, peak):
                    return functools.reduce(jnp.maximum, scores(t, 0.0, rows)[0], peak)

                peak = lax.fori_loop(0, turns, find_peak, jnp.full((SHARD, WIDTH), LOW, F32))
                top = jnp.broadcast_to(jnp.max(peak, axis=1, keepdims=True), (SHARD, WIDTH))
                shift_ref[:, rows] = top.T[:16]

                def add_up(t, carry):
                    parts, key = scores(t, 0.0, rows)
                    add([part - top for part in parts], key, rows)
                    return carry

                return lax.fori_loop(0, turns, add_up, carry)

            lax.fori_loop(0, helpers, one_part, 0)

        whole = sum_ref[...]
        hi = whole.astype(BF16)
        mid = (whole - hi.astype(F32)).astype(BF16)
        ones = jnp.ones((WIDTH, WIDTH), BF16)
        across = jnp.dot(hi, ones, preferred_element_type=F32) + jnp.dot(mid, ones, preferred_element_type=F32)
        mean = (acc_ref[...] * (1.0 / across)).astype(BF16)
        few = jnp.ones((16, WIDTH), BF16)
        total = lax.dot_general(few, hi, LANES, preferred_element_type=F32)
        total += lax.dot_general(few, mid, LANES, preferred_element_type=F32)
        lse = in_three(shift_ref[...] + jnp.log(total)).astype(BF16)
        for c in range(helpers):
            rows = slice(c * SHARD, (c + 1) * SHARD)
            out_ref, to = out_refs[c % CS], c // CS
            out_ref[to, pl.ds(q_at, SHARD), :] = mean[rows]
            out_ref[to, pl.ds(pl.multiple_of(q_at + SHARD, 16), 16), :] = lse[:, rows]
        return carry

    lax.fori_loop(0, 2, one_side, 0)


def merge_kernel(own_ref, other_ref, *refs):
    *out_refs, scr_ref = refs
    cases = [(k, side * SIDE) for k in range(len(out_refs)) for side in range(2)]
    scr_ref[...] = jnp.zeros(scr_ref.shape, F32)
    for n, (k, at) in enumerate(cases):
        own = of_three(own_ref[k, pl.ds(at + SHARD, 16), :])
        other = of_three(other_ref[k, pl.ds(at + SHARD, 16), :])
        top = jnp.maximum(own, other)
        share = jnp.exp(own - top)
        total = share + jnp.exp(other - top)
        scr_ref[pl.ds(n, 1), :] = share / total
        lse = jnp.broadcast_to(top + jnp.log(total), (16, SHARD))
        out_refs[k][pl.ds(at + SHARD, 16), :] = in_three(lse).astype(BF16)
    columns = scr_ref[...].T
    for n, (k, at) in enumerate(cases):
        own = own_ref[k, pl.ds(at, SHARD), :].astype(F32)
        other = other_ref[k, pl.ds(at, SHARD), :].astype(F32)
        out_refs[k][pl.ds(at, SHARD), :] = (other + columns[:, n : n + 1] * (own - other)).astype(BF16)


def settle_kernel(*refs):
    got_refs, refs = refs[:YS], refs[YS:]
    tp_ref, sp_ref, ntp_ref, level_ref, nsp_ref, *msg_refs, scr_ref = refs
    for side, old_ref, new_ref in ((0, tp_ref, ntp_ref), (1, sp_ref, nsp_ref)):
        at = side * SIDE
        parts = [of_three(ref[pl.ds(at + SHARD, 16), :]) for ref in got_refs]
        top = functools.reduce(jnp.maximum, parts)
        shares = [jnp.exp(part - top) for part in parts]
        total = functools.reduce(jnp.add, shares)
        scr_ref[...] = jnp.zeros(scr_ref.shape, F32)
        for h, share in enumerate(shares):
            scr_ref[pl.ds(h, 1), :] = share / total
        columns = scr_ref[...].T
        mean = jnp.zeros((SHARD, WIDTH), F32)
        for h, ref in enumerate(got_refs):
            mean = mean + columns[:, h : h + 1] * ref[pl.ds(at, SHARD), :].astype(F32)
        old = old_ref[pl.ds(0, SHARD), :]
        square = square_row(old.astype(BF16))
        level = -TEMPER * (top + jnp.log(total) - square * (1.0 / (WIDTH * TEMPER)))
        new = old + STRIDE * (mean - old)
        new_ref[pl.ds(0, SHARD), :] = new
        if side:
            new_ref[pl.ds(SHARD, 8), :] = level[:8]
        else:
            level_ref[...] = level[:1]
        if msg_refs:
            write_side(*msg_refs, side, new, level)


def finish_kernel(at_ref, *refs):
    own_ref, other_ref, points_ref, level_ref = refs
    for n in range(YS * CS):
        ref = (own_ref, other_ref)[n % CS].at[n // CS]
        helper = ((at_ref[2] - n // CS) & (YS - 1)) * CS + ((at_ref[3] + n) & (CS - 1))
        points_ref[0, pl.ds(pl.multiple_of(helper * SHARD, SHARD), SHARD), :] = ref[pl.ds(0, SHARD), :]
        level_ref[pl.ds(helper, 1), :] = ref[pl.ds(SHARD, 1), :]


def near_core(*arrays):
    return [pltpu.with_memory_space_constraint(x, pltpu.VMEM) for x in arrays]


def exchanged(copies, axes):
    return lax.all_to_all(copies, axes, split_axis=0, concat_axis=0, tiled=True)


def shifted(x, axis, step):
    n = lax.axis_size(axis)
    return lax.ppermute(x, axis, [(i, (i + step) % n) for i in range(n)])


def crossed(x, axis, bit):
    return lax.ppermute(x, axis, [(i, i ^ bit) for i in range(lax.axis_size(axis))])


def from_helpers(msg):
    near = jnp.stack([msg, crossed(msg, "c", 1)])
    near = jnp.concatenate([near, crossed(near, "y", 1)])
    return near, crossed(near, "y", 2)


def from_helpers_late(msg):
    parts = [msg]
    for k in range(1, YS):
        parts.append(shifted(msg, "y", k))
    own = jnp.stack(parts)
    return own, shifted(own, "c", 1)


def from_blocks(copies, source):
    sides = [source]
    for k in range(1, XS):
        sides.append(shifted(source, "x", k))
    near = exchanged(copies, "z")
    ring = [None] * ZS
    ring[0] = ahead = back = jnp.stack(sides)
    targets = [near]
    for k in range(1, XS):
        targets.append(shifted(near, "x", k))
    for k in range(1, ZS // 2 + 1):
        ring[k] = ahead = shifted(ahead, "z", 1)
        if k < ZS // 2:
            ring[ZS - k] = back = shifted(back, "z", ZS - 1)
    return targets, ring


def on_device(
    source_points, source_potential, target_points, target_potential, pairs, counts, owner
):
    helper = lax.axis_index(HELP)
    block = lax.axis_index(("x", "z"))
    blocks = XS * ZS
    helpers = YS * CS
    at = jnp.stack([lax.axis_index(axis) for axis in ("x", "z", "y", "c")])
    smem = pl.BlockSpec(memory_space=pltpu.SMEM)
    vmem = pl.BlockSpec(memory_space=pltpu.VMEM)
    msg_shape = pltpu.VMEM((MSG, WIDTH), BF16)
    copies_shape = pltpu.VMEM((ZS, SIDE, WIDTH), BF16)
    source_shape = pltpu.VMEM((SIDE, WIDTH), BF16)
    half_shape = pltpu.VMEM((YS, MSG, WIDTH), BF16)
    final_shape = pltpu.VMEM((SHARD + 8, WIDTH), F32)
    own_points = pl.BlockSpec((1, SHARD, WIDTH), lambda i, at: (0, at[0], 0))
    own_level = pl.BlockSpec((1, SHARD), lambda i, at: (0, at[0]))
    whole = lambda *shape: pl.BlockSpec(shape, lambda i, at: (0,) * len(shape))
    msg, copies, source = pl.pallas_call(
        prepare_kernel,
        out_shape=(msg_shape, copies_shape, source_shape),
        grid_spec=pltpu.PrefetchScalarGridSpec(
            num_scalar_prefetch=1,
            grid=(1,),
            in_specs=[smem, smem, smem, whole(1, SHARD, WIDTH), whole(1, SHARD), own_points, own_level],
            out_specs=(whole(*msg_shape.shape), whole(*copies_shape.shape), whole(*source_shape.shape)),
        ),
        name="prepare",
    )(helper[None], pairs, counts, owner, target_points, target_potential, source_points, source_potential)
    tp = target_points[0]
    sp = lax.dynamic_slice_in_dim(source_points[0], helper * SHARD, SHARD, 0)
    points_shape = jax.ShapeDtypeStruct((SHARD, WIDTH), F32)
    kept_shape = pltpu.VMEM((SHARD, WIDTH), F32)
    level_shape = jax.ShapeDtypeStruct((1, SHARD), F32)
    named = None
    for step in range(ITERS):
        targets, sources = from_blocks(copies, source)
        query = from_helpers(msg)
        if named is None:
            meta = jnp.concatenate([part[:, SHARD + META, :blocks] for part in targets])
            named = lax.dynamic_index_in_dim(meta, block, 1, False).astype(jnp.int32)
        own, other = pl.pallas_call(
            attend_kernel,
            out_shape=(half_shape, half_shape),
            in_specs=[smem] * 5 + [vmem] * (XS + ZS + 2),
            out_specs=(vmem, vmem),
            scratch_shapes=[
                pltpu.SMEM((2, blocks + GROUP), jnp.int32),
                pltpu.VMEM((2 * blocks, SIDE, WIDTH), BF16),
                pltpu.VMEM((helpers * SHARD, WIDTH), BF16),
                pltpu.VMEM((16, helpers * SHARD), F32),
                pltpu.VMEM((helpers * SHARD, WIDTH), F32),
                pltpu.VMEM((helpers * SHARD, WIDTH), F32),
            ],
            name="attend",
        )(
            at, pairs, counts, owner, named,
            targets[0], *near_core(*targets[1:]),
            *sources[: ZS // 2], *near_core(*sources[ZS // 2 : ZS // 2 + 2]), *sources[ZS // 2 + 2 :],
            query[0], *near_core(*query[1:]),
        )
        other = shifted(other, "c", 1)
        merged = pl.pallas_call(
            merge_kernel,
            out_shape=(msg_shape,) * YS,
            in_specs=[vmem, vmem],
            out_specs=(vmem,) * YS,
            scratch_shapes=[pltpu.VMEM((WIDTH, SHARD), F32)],
            name="merge",
        )(*near_core(own, other))
        got = [merged[0]]
        for k in range(1, YS):
            got.append(crossed(merged[k], "y", k))
        last = step == ITERS - 1
        messages = () if last else (msg_shape, copies_shape, source_shape)
        tp, tl, sp, *rest = pl.pallas_call(
            settle_kernel,
            out_shape=(points_shape if last else kept_shape, level_shape, final_shape, *messages),
            in_specs=[vmem] * (YS + 2),
            out_specs=(vmem,) * (3 + len(messages)),
            scratch_shapes=[pltpu.VMEM((WIDTH, SHARD), F32)],
            name="settle",
        )(*near_core(*got), *((tp, sp) if step == 0 else near_core(tp, sp)))
        msg, copies, source = rest or (None,) * 3
    pieces = near_core(*from_helpers_late(sp))
    new_source_points, new_source_potential = pl.pallas_call(
        finish_kernel,
        out_shape=(jax.ShapeDtypeStruct(source_points.shape, F32), jax.ShapeDtypeStruct((helpers, SHARD), F32)),
        in_specs=[smem, vmem, vmem],
        out_specs=(vmem, vmem),
        name="finish",
    )(at, *pieces)
    return new_source_points, new_source_potential.reshape(source_potential.shape), tp[None], tl


def solution(mesh):
    torus = Mesh(mesh.devices.reshape(XS, ZS, YS, CS), ("x", "z", "y", "c"))
    blk = ("x", "z")
    in_specs = (
        P(blk, None, None),
        P(blk, None),
        P(blk, HELP, None),
        P(blk, HELP),
        P(blk, None),
        P(blk),
        P(),
    )
    out_specs = (P(blk, None, None), P(blk, None), P(blk, HELP, None), P(blk, HELP))
    return jax.shard_map(
        on_device, mesh=torus, in_specs=in_specs, out_specs=out_specs, check_vma=False
    )
```
